32 devices in a mesh: dp: 2 (over x), ep: 16 (over z, y, core).
Axes of the slice: x: 2, y: 2, z: 4, core: 2. Of those that a mesh axis runs over, the one named last changes fastest.
Arguments:
- hidden_state: bfloat16 [4096, 1024], P(('dp', 'ep')), parts along dimension 0
- key_cache: bfloat16 [2, 4096, 32, 8, 64], P(None, ('dp', 'ep')), parts along dimension 1
- value_cache: bfloat16 [2, 4096, 32, 8, 64], P(None, ('dp', 'ep')), parts along dimension 1
- positions: int32 [4096], P(('dp', 'ep')), parts along dimension 0
- expert_ids: int32 [2, 4096, 8], P(None, ('dp', 'ep')), parts along dimension 1
- attn_gain: float32 [2, 1024], replicated
- w_query: bfloat16 [2, 1024, 1024], replicated
- w_key: bfloat16 [2, 1024, 512], replicated
- w_value: bfloat16 [2, 1024, 512], replicated
- q_gain: float32 [2, 1024], replicated
- k_gain: float32 [2, 512], replicated
- w_out: bfloat16 [2, 1024, 1024], replicated
- moe_gain: float32 [2, 1024], replicated
- w_router: bfloat16 [2, 1024, 32], replicated
- w_gate: bfloat16 [2, 32, 1024, 512], P(None, 'ep')
- w_up: bfloat16 [2, 32, 1024, 512], P(None, 'ep')
- w_down: bfloat16 [2, 32, 512, 1024], P(None, 'ep')
Outputs:
- output 1: bfloat16 [4096, 1024], P(('dp', 'ep')), parts along dimension 0
- output 2: bfloat16 [2, 4096, 32, 8, 64], P(None, ('dp', 'ep')), parts along dimension 1
- output 3: bfloat16 [2, 4096, 32, 8, 64], P(None, ('dp', 'ep')), parts along dimension 1
There are 2 independent parts. The reference program is written for one: setup_inputs(seed, part) draws one part's arguments, and reference() takes and returns one part's arrays. A program takes and returns all parts, laid end to end along the dimension named above; an argument that names none is the same for every part.
All inputs are finite; a program needn't handle non-finite values.
Results may differ from the reference program's by a relative error of at most 0.0191773.
Values are sent between devices in bfloat16 or wider.
A program may use at most 1 GiB of HBM per device.

```python
import jax
import jax.numpy as jnp
from jax import lax

HIDDEN = 1024
HEADS = 16
KV_HEADS = 8
HEAD_DIM = 64
EXPERTS = 32
TOP_K = 8
EXPERT_FF = 512
BATCH_DEV = 128
SLOTS = 32
GROUP = 16
LAYERS = 2
BATCH = BATCH_DEV * GROUP
LOCAL_EXPERTS = EXPERTS // GROUP
CAP = (4 * BATCH_DEV * TOP_K + EXPERTS - 1) // EXPERTS
EXPERT_ROWS = GROUP * CAP
Q_WIDTH = HEADS * HEAD_DIM
KV_WIDTH = KV_HEADS * HEAD_DIM
NORM_EPS = 1e-5
ROPE_THETA = 10000.0


def scaled_normal(rng_key, shape, scale):
    return (jax.random.normal(rng_key, shape, jnp.float32) * scale).astype(jnp.bfloat16)


def draw_positions(rng_key):
    k_len, k_pick = jax.random.split(rng_key)
    drawn = jax.random.randint(k_len, (BATCH,), 0, SLOTS)
    longest = jax.random.randint(k_pick, (), 0, BATCH)
    return jnp.where(jnp.arange(BATCH) == longest, SLOTS - 1, drawn).astype(jnp.int32)


def draw_routes(rng_key):
    hot_n = EXPERTS // 16
    row_total = BATCH_DEV * TOP_K
    rest_rows = row_total - hot_n * CAP
    cold_n = EXPERTS - hot_n
    rank_ids = jnp.arange(EXPERTS)
    counts = jnp.where(rank_ids < hot_n, CAP, rest_rows // cold_n + (rank_ids - hot_n < rest_rows % cold_n).astype(jnp.int32))
    run_ends = jnp.cumsum(counts)
    spot_ids = jnp.arange(row_total)
    rank_at = jnp.sum((spot_ids[:, None] >= run_ends[None, :]).astype(jnp.int32), axis=1)
    rank_grid = rank_at.reshape(TOP_K, BATCH_DEV).T

    def one_layer(layer_key):
        k_dev, k_loc, k_src = jax.random.split(layer_key, 3)
        dev_order = jax.random.permutation(k_dev, GROUP)
        loc_order = jax.random.permutation(k_loc, LOCAL_EXPERTS)
        base_order = (dev_order[:, None] * LOCAL_EXPERTS + loc_order[None, :]).reshape(-1)

        def one_source(src_key):
            k_cold, k_tok, k_pick = jax.random.split(src_key, 3)
            cold_perm = jax.random.permutation(k_cold, cold_n)
            expert_order = jnp.concatenate([base_order[:hot_n], base_order[hot_n:][cold_perm]])
            chosen = expert_order[rank_grid][jax.random.permutation(k_tok, BATCH_DEV)]
            scores = jax.random.randint(k_pick, (BATCH_DEV, TOP_K), 0, 1024) * TOP_K + jnp.arange(TOP_K)
            return jnp.take_along_axis(chosen, jnp.argsort(scores, axis=1), axis=1)

        return jax.vmap(one_source)(jax.random.split(k_src, GROUP)).reshape(BATCH, TOP_K)

    return jax.vmap(one_layer)(jax.random.split(rng_key, LAYERS)).astype(jnp.int32)


def setup_inputs(seed: int = 0, part: int = 0) -> dict:
    part_key = jax.random.fold_in(jax.random.key(seed), part)
    k_hidden, k_keys, k_values, k_pos, k_route = jax.random.split(part_key, 5)
    shared_keys = jax.random.split(jax.random.key(seed + 1), 12)
    hidden_scale = HIDDEN ** -0.5
    cache_shape = (LAYERS, BATCH, SLOTS, KV_HEADS, HEAD_DIM)
    return {
        'hidden_state': scaled_normal(k_hidden, (BATCH, HIDDEN), 1.0),
        'key_cache': scaled_normal(k_keys, cache_shape, 1.0),
        'value_cache': scaled_normal(k_values, cache_shape, 1.0),
        'positions': draw_positions(k_pos),
        'expert_ids': draw_routes(k_route),
        'attn_gain': jax.random.uniform(shared_keys[0], (LAYERS, HIDDEN), jnp.float32, 0.6, 1.6),
        'w_query': scaled_normal(shared_keys[1], (LAYERS, HIDDEN, Q_WIDTH), hidden_scale),
        'w_key': scaled_normal(shared_keys[2], (LAYERS, HIDDEN, KV_WIDTH), hidden_scale),
        'w_value': scaled_normal(shared_keys[3], (LAYERS, HIDDEN, KV_WIDTH), hidden_scale),
        'q_gain': jax.random.uniform(shared_keys[4], (LAYERS, Q_WIDTH), jnp.float32, 0.8, 2.0),
        'k_gain': jax.random.uniform(shared_keys[5], (LAYERS, KV_WIDTH), jnp.float32, 0.8, 2.0),
        'w_out': scaled_normal(shared_keys[6], (LAYERS, Q_WIDTH, HIDDEN), 2.0 * Q_WIDTH ** -0.5),
        'moe_gain': jax.random.uniform(shared_keys[7], (LAYERS, HIDDEN), jnp.float32, 0.6, 1.6),
        'w_router': scaled_normal(shared_keys[8], (LAYERS, HIDDEN, EXPERTS), 2.0 * hidden_scale),
        'w_gate': scaled_normal(shared_keys[9], (LAYERS, EXPERTS, HIDDEN, EXPERT_FF), hidden_scale),
        'w_up': scaled_normal(shared_keys[10], (LAYERS, EXPERTS, HIDDEN, EXPERT_FF), hidden_scale),
        'w_down': scaled_normal(shared_keys[11], (LAYERS, EXPERTS, EXPERT_FF, HIDDEN), 0.5 * (EXPERTS / EXPERT_FF) ** 0.5),
    }


def rms_scale(tensor, gain):
    mean_sq = jnp.mean(tensor * tensor, axis=-1, keepdims=True)
    return tensor * lax.rsqrt(mean_sq + NORM_EPS) * gain


def rotate_heads(tensor, positions):
    half_dim = HEAD_DIM // 2
    inv_freq = ROPE_THETA ** (-jnp.arange(0, HEAD_DIM, 2, dtype=jnp.float32) / HEAD_DIM)
    angles = positions.astype(jnp.float32)[:, None] * inv_freq[None, :]
    angles = jnp.concatenate([angles, angles], axis=-1)[:, None, :]
    turned = jnp.concatenate([-tensor[..., half_dim:], tensor[..., :half_dim]], axis=-1)
    return tensor * jnp.cos(angles) + turned * jnp.sin(angles)


def attention_layer(hidden_x, key_l, value_l, positions, attn_gain, w_query, w_key, w_value, q_gain, k_gain, w_out):
    normed = rms_scale(hidden_x.astype(jnp.float32), attn_gain).astype(jnp.bfloat16)
    query_rot = rms_scale(jnp.dot(normed, w_query, preferred_element_type=jnp.float32), q_gain)
    query_rot = rotate_heads(query_rot.reshape(BATCH, HEADS, HEAD_DIM), positions).astype(jnp.bfloat16)
    key_new = rms_scale(jnp.dot(normed, w_key, preferred_element_type=jnp.float32), k_gain)
    key_new = rotate_heads(key_new.reshape(BATCH, KV_HEADS, HEAD_DIM), positions).astype(jnp.bfloat16)
    value_new = jnp.dot(normed, w_value, preferred_element_type=jnp.float32).astype(jnp.bfloat16).reshape(BATCH, KV_HEADS, HEAD_DIM)
    slot_ids = jnp.arange(SLOTS)
    at_pos = (slot_ids[None, :] == positions[:, None])[:, :, None, None]
    key_l = jnp.where(at_pos, key_new[:, None], key_l)
    value_l = jnp.where(at_pos, value_new[:, None], value_l)
    grouped = query_rot.reshape(BATCH, KV_HEADS, HEADS // KV_HEADS, HEAD_DIM)
    scores = jnp.einsum('bkgh,bskh->bkgs', grouped.astype(jnp.float32), key_l.astype(jnp.float32)) * HEAD_DIM ** -0.5
    visible = (slot_ids[None, :] <= positions[:, None])[:, None, None, :]
    attn_probs = jax.nn.softmax(jnp.where(visible, scores, -jnp.inf), axis=-1).astype(jnp.bfloat16)
    attended = jnp.einsum('bkgs,bskh->bkgh', attn_probs.astype(jnp.float32), value_l.astype(jnp.float32)).astype(jnp.bfloat16)
    attn_out = jnp.dot(attended.reshape(BATCH, Q_WIDTH), w_out, preferred_element_type=jnp.float32)
    return (hidden_x.astype(jnp.float32) + attn_out).astype(jnp.bfloat16), key_l, value_l


def moe_layer(hidden_x, choice_ids, moe_gain, w_router, w_gate, w_up, w_down):
    normed = rms_scale(hidden_x.astype(jnp.float32), moe_gain).astype(jnp.bfloat16)
    probs = jax.nn.softmax(jnp.dot(normed, w_router, preferred_element_type=jnp.float32), axis=-1)
    gate_vals = jnp.take_along_axis(probs, choice_ids, axis=1)
    flat_ids = choice_ids.reshape(-1)
    sort_order = jnp.argsort(flat_ids, stable=True)
    sorted_ids = flat_ids[sort_order]
    starts = jnp.searchsorted(sorted_ids, jnp.arange(EXPERTS))
    padded_rows = jnp.concatenate([normed[sort_order // TOP_K], jnp.zeros((EXPERT_ROWS, HIDDEN), jnp.bfloat16)])

    def run_expert(expert):
        row_block = lax.dynamic_slice_in_dim(padded_rows, starts[expert], EXPERT_ROWS)
        gate_part = jnp.dot(row_block, w_gate[expert], preferred_element_type=jnp.float32)
        up_part = jnp.dot(row_block, w_up[expert], preferred_element_type=jnp.float32)
        activated = (jax.nn.silu(gate_part) * up_part).astype(jnp.bfloat16)
        return jnp.dot(activated, w_down[expert], preferred_element_type=jnp.float32).astype(jnp.bfloat16)

    expert_out = lax.map(run_expert, jnp.arange(EXPERTS))
    in_sorted = expert_out[sorted_ids, jnp.arange(BATCH * TOP_K) - starts[sorted_ids]]
    picked = in_sorted[jnp.argsort(sort_order)].reshape(BATCH, TOP_K, HIDDEN)
    mixed_sum = jnp.sum(gate_vals[:, :, None] * picked.astype(jnp.float32), axis=1)
    return (hidden_x.astype(jnp.float32) + mixed_sum).astype(jnp.bfloat16)


def reference(hidden_state, key_cache, value_cache, positions, expert_ids, attn_gain, w_query, w_key, w_value, q_gain, k_gain, w_out, moe_gain, w_router, w_gate, w_up, w_down):
    hidden_x = hidden_state
    new_keys = []
    new_values = []
    for layer_idx in range(LAYERS):
        hidden_x, key_l, value_l = attention_layer(hidden_x, key_cache[layer_idx], value_cache[layer_idx], positions, attn_gain[layer_idx], w_query[layer_idx], w_key[layer_idx], w_value[layer_idx], q_gain[layer_idx], k_gain[layer_idx], w_out[layer_idx])
        new_keys.append(key_l)
        new_values.append(value_l)
        hidden_x = moe_layer(hidden_x, expert_ids[layer_idx], moe_gain[layer_idx], w_router[layer_idx], w_gate[layer_idx], w_up[layer_idx], w_down[layer_idx])
    return hidden_x, jnp.stack(new_keys), jnp.stack(new_values)
```

```python
import functools

import jax
import jax.numpy as jnp
from jax import lax
from jax.experimental import pallas as pl
from jax.experimental.pallas import tpu as pltpu
from jax.sharding import PartitionSpec as P

NORM_EPS = 1e-5
ROPE_THETA = 10000.0
F32 = jnp.float32
BF16 = jnp.bfloat16
MESH = pl.DeviceIdType.MESH
RS_SUBS = 4
AG_SUBS = 2
VMEM_LIMIT = 60 * 1024 * 1024


def rms_scale(tensor, gain):
    mean_sq = jnp.mean(tensor * tensor, axis=-1, keepdims=True)
    return tensor * lax.rsqrt(mean_sq + NORM_EPS) * gain


def attention_kernel(layer, x_ref, pos_ref, freq_ref, ids_ref, again_ref, qgain_ref, kgain_ref, mgain_ref, wr_ref, kc_hbm, vc_hbm, wq_hbm, wk_hbm, wv_hbm, wo_hbm, *rest):
    if layer:
        rest = rest[2:]
    (x_out, u_out, gate_out, ko_hbm, vo_hbm, wq, wk, wv, wo, kbuf, vbuf, q_rows, k_t, v_t, o_rows, cos_t, sin_t, score, w_sem, kin_sem, vin_sem, kout_sem, vout_sem) = rest
    heads, slots, dim, rows = kbuf.shape
    half = dim // 2
    w_copies = [pltpu.make_async_copy(src.at[layer], dst, w_sem.at[i]) for i, (src, dst) in enumerate(((wq_hbm, wq), (wk_hbm, wk), (wv_hbm, wv), (wo_hbm, wo)))]
    for copy in w_copies[:3]:
        copy.start()

    def cache_in(n):
        return (pltpu.make_async_copy(kc_hbm.at[layer, :, n], kbuf.at[n], kin_sem.at[n]), pltpu.make_async_copy(vc_hbm.at[layer, :, n], vbuf.at[n], vin_sem.at[n]))

    def cache_out(n):
        return (pltpu.make_async_copy(kbuf.at[n], ko_hbm.at[layer, :, n], kout_sem.at[n]), pltpu.make_async_copy(vbuf.at[n], vo_hbm.at[layer, :, n], vout_sem.at[n]))

    for n in range(heads):
        for copy in cache_in(n):
            copy.start()
    w_copies[3].start()

    pos = pos_ref[...]
    angles = pos.astype(F32) * freq_ref[...]
    cos_t[...] = jnp.cos(angles)
    sin_t[...] = jnp.sin(angles)
    normed = rms_scale(x_ref[...].astype(F32), again_ref[...]).astype(BF16)

    def rope(tensor):
        lo, hi = tensor[:half], tensor[half:]
        cos, sin = cos_t[...], sin_t[...]
        return jnp.concatenate([lo * cos - hi * sin, hi * cos + lo * sin], axis=0)

    w_copies[0].wait()
    q_rows[...] = rms_scale(jnp.dot(normed, wq[...], preferred_element_type=F32), qgain_ref[...])
    w_copies[1].wait()
    key_new = rms_scale(jnp.dot(normed, wk[...], preferred_element_type=F32), kgain_ref[...])
    w_copies[2].wait()
    value_new = jnp.dot(normed, wv[...], preferred_element_type=F32)
    pair = 2 * dim
    for c in range(heads // 2):
        chunk = key_new[:, c * pair:(c + 1) * pair].T
        for j in range(2):
            k_t[2 * c + j] = rope(chunk[j * dim:(j + 1) * dim]).astype(BF16)
        chunk = value_new[:, c * pair:(c + 1) * pair].T.astype(BF16)
        for j in range(2):
            v_t[2 * c + j] = chunk[j * dim:(j + 1) * dim]

    pos_b = jnp.broadcast_to(pos.astype(F32), (dim, rows)).astype(BF16)
    slot_ids = lax.broadcasted_iota(jnp.int32, (slots, rows), 0)

    def one_head(n, carry):
        cols = pl.ds(pl.multiple_of(n * pair, pair), pair)
        qt = q_rows[:, cols].T
        q0 = rope(qt[:dim]).astype(BF16).astype(F32) * dim ** -0.5
        q1 = rope(qt[dim:]).astype(BF16).astype(F32) * dim ** -0.5
        k_new, v_new = k_t[n], v_t[n]
        k_in, v_in = cache_in(n)
        k_in.wait()
        for s in range(slots):
            key = jnp.where(pos_b == s, k_new, kbuf[n, s])
            kbuf[n, s] = key
            key = key.astype(F32)
            score[0, s:s + 1] = jnp.sum(key * q0, axis=0, keepdims=True)
            score[1, s:s + 1] = jnp.sum(key * q1, axis=0, keepdims=True)
        k_out, v_out = cache_out(n)
        k_out.start()
        for g in range(2):
            masked = jnp.where(slot_ids <= pos, score[g], -jnp.inf)
            weight = jnp.exp(masked - jnp.max(masked, axis=0, keepdims=True))
            score[g] = (weight / jnp.sum(weight, axis=0, keepdims=True)).astype(BF16).astype(F32)
        v_in.wait()
        acc0 = jnp.zeros((dim, rows), F32)
        acc1 = jnp.zeros((dim, rows), F32)
        for s in range(slots):
            value = jnp.where(pos_b == s, v_new, vbuf[n, s])
            vbuf[n, s] = value
            value = value.astype(F32)
            acc0 += value * score[0, s:s + 1]
            acc1 += value * score[1, s:s + 1]
        v_out.start()
        o_rows[:, cols] = jnp.concatenate([acc0, acc1], axis=0).T.astype(BF16)
        return carry

    lax.fori_loop(0, heads, one_head, 0)
    w_copies[3].wait()
    x_new = (x_ref[...].astype(F32) + jnp.dot(o_rows[...], wo[...], preferred_element_type=F32)).astype(BF16)
    x_out[...] = x_new
    u = rms_scale(x_new.astype(F32), mgain_ref[...]).astype(BF16)
    u_out[...] = u
    logits = lax.dot_general(wr_ref[...], u, (((1,), (1,)), ((), ())), preferred_element_type=F32)
    weight = jnp.exp(logits - jnp.max(logits, axis=0, keepdims=True))
    probs = weight / jnp.sum(weight, axis=0, keepdims=True)
    expert_ids = lax.broadcasted_iota(jnp.int32, probs.shape, 0)
    member = expert_ids == ids_ref[0:1]
    for j in range(1, ids_ref.shape[0]):
        member = member | (expert_ids == ids_ref[j:j + 1])
    gate_out[...] = jnp.where(member, probs, 0.0)
    for n in range(heads):
        for copy in cache_out(n):
            copy.wait()


def attention_call(layer, x, pos, freq, ids, again, qgain, kgain, mgain, wr, kc, vc, wq, wk, wv, wo, prev):
    layers, slots, heads, dim, rows = kc.shape
    hidden = x.shape[1]
    experts = wr.shape[0]
    q_width, kv_width = wq.shape[2], wk.shape[2]
    vmem, hbm = pl.BlockSpec(memory_space=pltpu.VMEM), pl.BlockSpec(memory_space=pl.ANY)
    args = (x, pos, freq, ids, again, qgain, kgain, mgain, wr, kc, vc, wq, wk, wv, wo) + tuple(prev)
    return pl.pallas_call(
        functools.partial(attention_kernel, layer),
        name=f"attention_{layer}",
        out_shape=(
            jax.ShapeDtypeStruct((rows, hidden), BF16),
            jax.ShapeDtypeStruct((rows, hidden), BF16),
            jax.ShapeDtypeStruct((experts, rows), F32),
            jax.ShapeDtypeStruct(kc.shape, kc.dtype),
            jax.ShapeDtypeStruct(vc.shape, vc.dtype),
        ),
        in_specs=[vmem] * 9 + [hbm] * (len(args) - 9),
        out_specs=(vmem, vmem, vmem, hbm, hbm),
        scratch_shapes=[
            pltpu.VMEM((hidden, q_width), BF16),
            pltpu.VMEM((hidden, kv_width), BF16),
            pltpu.VMEM((hidden, kv_width), BF16),
            pltpu.VMEM((q_width, hidden), BF16),
            pltpu.VMEM((heads, slots, dim, rows), BF16),
            pltpu.VMEM((heads, slots, dim, rows), BF16),
            pltpu.VMEM((rows, q_width), F32),
            pltpu.VMEM((heads, dim, rows), BF16),
            pltpu.VMEM((heads, dim, rows), BF16),
            pltpu.VMEM((rows, q_width), BF16),
            pltpu.VMEM((dim // 2, rows), F32),
            pltpu.VMEM((dim // 2, rows), F32),
            pltpu.VMEM((2, slots, rows), F32),
            pltpu.SemaphoreType.DMA((4,)),
            pltpu.SemaphoreType.DMA((heads,)),
            pltpu.SemaphoreType.DMA((heads,)),
            pltpu.SemaphoreType.DMA((heads,)),
            pltpu.SemaphoreType.DMA((heads,)),
        ],
        input_output_aliases={15: 3, 16: 4} if prev else {},
        compiler_params=pltpu.CompilerParams(vmem_limit_bytes=VMEM_LIMIT),
    )(*args)


def moe_kernel(layer, u_ref, gate_ref, x_ref, wg_hbm, wu_hbm, wd_hbm, out_ref, wg, wu, wd, ag_u, ag_g, part, psib, rs_in, w_sem, agu_send, agu_recv, sbu_send, sbu_recv, agg_send, agg_recv, sbg_send, sbg_recv, ps_send, ps_recv, rs_send, rs_recv):
    steps, _, rows, hidden = part.shape
    me = lax.axis_index("ep")
    core, chip = me % 2, me // 2
    chip_z, chip_y = chip // 2, chip % 2
    place = chip_y * (steps - 1 - chip_z) + (1 - chip_y) * chip_z

    def device_at(p, c):
        far = p // (steps // 2)
        z = (1 - far) * p + far * (steps - 1 - p)
        return (z * 2 + far) * 2 + c

    nxt = device_at((place + 1 - 2 * core + steps) % steps, core)
    prv = device_at((place - 1 + 2 * core + steps) % steps, core)
    sib = chip * 2 + (1 - core)

    w_copies = [pltpu.make_async_copy(src.at[layer], dst, w_sem.at[i]) for i, (src, dst) in enumerate(((wg_hbm, wg), (wu_hbm, wu), (wd_hbm, wd)))]
    for copy in w_copies:
        copy.start()
    barrier = pltpu.get_barrier_semaphore()
    for peer in (prv, sib):
        pl.semaphore_signal(barrier, inc=1, device_id={"ep": peer}, device_id_type=MESH)

    def remote(src, dst, send, recv, peer):
        return pltpu.make_async_remote_copy(src_ref=src, dst_ref=dst, send_sem=send, recv_sem=recv, device_id={"ep": peer}, device_id_type=MESH)

    ag_rows = rows // AG_SUBS
    rs_rows = rows // RS_SUBS

    def ring_u(k, s, src=None):
        span = pl.ds(s * ag_rows, ag_rows)
        src = ag_u.at[k, 0, span] if src is None else src.at[span]
        return remote(src, ag_u.at[k + 1, 0, span], agu_send.at[k, s], agu_recv.at[k + 1, s], nxt)

    def sib_u(k, s, src=None):
        span = pl.ds(s * ag_rows, ag_rows)
        src = ag_u.at[k, 0, span] if src is None else src.at[span]
        return remote(src, ag_u.at[k, 1, span], sbu_send.at[k, s], sbu_recv.at[k, s], sib)

    def ring_g(k, src=None):
        return remote(ag_g.at[k, 0] if src is None else src, ag_g.at[k + 1, 0], agg_send.at[k], agg_recv.at[k + 1], nxt)

    def sib_g(k, src=None):
        return remote(ag_g.at[k, 0] if src is None else src, ag_g.at[k, 1], sbg_send.at[k], sbg_recv.at[k], sib)

    def sib_part(k, s):
        span = pl.ds(s * rs_rows, rs_rows)
        return remote(part.at[k, 1, span], psib.at[k, span], ps_send.at[k, s], ps_recv.at[k, s], sib)

    def ring_part(k, s):
        span = pl.ds(s * rs_rows, rs_rows)
        return remote(part.at[k, 0, span], rs_in.at[k, span], rs_send.at[k, s], rs_recv.at[k, s], nxt)

    pl.semaphore_wait(barrier, 2)
    ring_g(0, gate_ref).start()
    for s in range(AG_SUBS):
        ring_u(0, s, u_ref).start()
    sib_g(0, gate_ref).start()
    for s in range(AG_SUBS):
        sib_u(0, s, u_ref).start()
    ag_u[0, 0] = u_ref[...]
    ag_g[0, 0] = gate_ref[...]

    def take_block(k):
        ring_g(k - 1).wait_recv()

        @pl.when(k < steps - 1)
        def _():
            ring_g(k).start()

        sib_g(k).start()
        for s in range(AG_SUBS):
            ring_u(k - 1, s).wait_recv()

            @pl.when(k < steps - 1)
            def _():
                ring_u(k, s).start()

            sib_u(k, s).start()

    def add_sub(k, s, first):
        span = pl.ds(s * rs_rows, rs_rows)
        sib_part(k, s).wait_recv()
        total = part[k, 0, span] + psib[k, span]
        if not first:
            ring_part(k - 1, s).wait_recv()
            total += rs_in[k - 1, span]
        part[k, 0, span] = total
        ring_part(k, s).start()

    lane = lax.broadcasted_iota(jnp.int32, (rows, gate_ref.shape[0]), 1)
    for copy in w_copies:
        copy.wait()

    def one_step(k, carry):
        sib_g(k).wait_recv()
        for s in range(AG_SUBS):
            sib_u(k, s).wait_recv()
        block = ag_u[k].reshape(2 * rows, hidden)
        gates = [ag_g[k, j].T for j in range(2)]
        piece = 0

        def reduce_piece(s):
            @pl.when(k == 2)
            def _():
                add_sub(k - 1, s, True)

            @pl.when(k > 2)
            def _():
                add_sub(k - 1, s, False)

        for e in range(2):
            gate_part = jnp.dot(block, wg[e], preferred_element_type=F32)
            up_part = jnp.dot(block, wu[e], preferred_element_type=F32)
            weight = jnp.concatenate([jnp.sum(jnp.where(lane == 2 * me + e, g, 0.0), axis=1, keepdims=True) for g in gates], axis=0)
            activated = jnp.where(weight != 0.0, jax.nn.silu(gate_part) * up_part, 0.0).astype(BF16)
            reduce_piece(2 * e)
            if e == 1:
                @pl.when(k < steps - 1)
                def _():
                    take_block(k + 1)

            expert_out = jnp.dot(activated, wd[e], preferred_element_type=F32).astype(BF16).astype(F32) * weight
            expert_out = expert_out.reshape(2, rows, hidden)
            if e == 0:
                part[k] = expert_out
            else:
                part[k] += expert_out
            reduce_piece(2 * e + 1)
        for s in range(RS_SUBS):
            sib_part(k, s).start()
        return carry

    lax.fori_loop(0, steps, one_step, 0)
    for s in range(RS_SUBS):
        add_sub(steps - 1, s, False)
    for s in range(RS_SUBS):
        span = pl.ds(s * rs_rows, rs_rows)
        sib_part(0, s).wait_recv()
        own = part[0, 0, span] + psib[0, span]
        ring_part(steps - 1, s).wait_recv()
        out_ref[span] = (x_ref[span].astype(F32) + (own + rs_in[steps - 1, span])).astype(BF16)

    def drain(k, carry):
        sib_g(k).wait_send()
        for s in range(AG_SUBS):
            sib_u(k, s).wait_send()
        for s in range(RS_SUBS):
            sib_part(k, s).wait_send()

        @pl.when(k < steps - 1)
        def _():
            ring_g(k).wait_send()
            for s in range(AG_SUBS):
                ring_u(k, s).wait_send()
            for s in range(RS_SUBS):
                ring_part(k + 1, s).wait_send()

        return carry

    lax.fori_loop(0, steps, drain, 0)


def moe_call(layer, u, gate, x, wg, wu, wd, steps):
    rows, hidden = u.shape
    experts = gate.shape[0]
    width = wg.shape[3]
    vmem, hbm = pl.BlockSpec(memory_space=pltpu.VMEM), pl.BlockSpec(memory_space=pl.ANY)
    dma = pltpu.SemaphoreType.DMA
    return pl.pallas_call(
        functools.partial(moe_kernel, layer),
        name=f"moe_{layer}",
        out_shape=jax.ShapeDtypeStruct((rows, hidden), BF16),
        in_specs=[vmem] * 3 + [hbm] * 3,
        out_specs=vmem,
        scratch_shapes=[
            pltpu.VMEM((2, hidden, width), BF16),
            pltpu.VMEM((2, hidden, width), BF16),
            pltpu.VMEM((2, width, hidden), BF16),
            pltpu.VMEM((steps, 2, rows, hidden), BF16),
            pltpu.VMEM((steps, 2, experts, rows), F32),
            pltpu.VMEM((steps, 2, rows, hidden), F32),
            pltpu.VMEM((steps, rows, hidden), F32),
            pltpu.VMEM((steps, rows, hidden), F32),
            dma((3,)),
            dma((steps, AG_SUBS)), dma((steps, AG_SUBS)), dma((steps, AG_SUBS)), dma((steps, AG_SUBS)),
            dma((steps,)), dma((steps,)), dma((steps,)), dma((steps,)),
            dma((steps, RS_SUBS)), dma((steps, RS_SUBS)), dma((steps, RS_SUBS)), dma((steps, RS_SUBS)),
        ],
        compiler_params=pltpu.CompilerParams(vmem_limit_bytes=VMEM_LIMIT, collective_id=layer, has_side_effects=True),
    )(u, gate, x, wg, wu, wd)


def solution(mesh):
    group_size = mesh.shape['ep']
    seq_axes = ('dp', 'ep')

    def device_step(hidden_state, key_cache, value_cache, positions, expert_ids, attn_gain, w_query, w_key, w_value, q_gain, k_gain, w_out, moe_gain, w_router, w_gate, w_up, w_down):
        dim = key_cache.shape[-1]
        rows = hidden_state.shape[0]
        freq = ROPE_THETA ** (-jnp.arange(0, dim, 2, dtype=F32) / dim)
        freq = jnp.broadcast_to(freq[:, None], (dim // 2, rows))
        keys = jnp.transpose(key_cache, (0, 2, 3, 4, 1))
        values = jnp.transpose(value_cache, (0, 2, 3, 4, 1))
        ids = jnp.transpose(expert_ids, (0, 2, 1))
        router = jnp.transpose(w_router, (0, 2, 1))
        pos = positions[None, :]
        hidden_x = hidden_state
        prev = ()
        for layer in range(key_cache.shape[0]):
            row = slice(layer, layer + 1)
            hidden_x, u, gate, *prev = attention_call(layer, hidden_x, pos, freq, ids[layer], attn_gain[row], q_gain[row], k_gain[row], moe_gain[row], router[layer], keys, values, w_query, w_key, w_value, w_out, prev)
            hidden_x = moe_call(layer, u, gate, hidden_x, w_gate, w_up, w_down, group_size // 2)
        return hidden_x, jnp.transpose(prev[0], (0, 4, 1, 2, 3)), jnp.transpose(prev[1], (0, 4, 1, 2, 3))

    cache_spec = P(None, seq_axes, None, None, None)
    expert_spec = P(None, 'ep', None, None)
    in_specs = (P(seq_axes, None), cache_spec, cache_spec, P(seq_axes), P(None, seq_axes, None)) + (P(),) * 9 + (expert_spec,) * 3
    out_specs = (P(seq_axes, None), cache_spec, cache_spec)
    return jax.shard_map(device_step, mesh=mesh, in_specs=in_specs, out_specs=out_specs, check_vma=False)
```

```python
import functools

import jax
import jax.numpy as jnp
from jax import lax
from jax.experimental import pallas as pl
from jax.experimental.pallas import tpu as pltpu
from jax.sharding import PartitionSpec as P
import numpy as np

NORM_EPS = 1e-5
ROPE_THETA = 10000.0
F32 = jnp.float32
BF16 = jnp.bfloat16
MESH = pl.DeviceIdType.MESH
RS_SUBS = 4
AG_SUBS = 4
ATTENTION_VMEM = 16 * 1024 * 1024
MOE_VMEM = 32 * 1024 * 1024


def rms_scale(tensor, gain):
    mean_sq = jnp.mean(tensor * tensor, axis=-1, keepdims=True)
    return tensor * lax.rsqrt(mean_sq + NORM_EPS) * gain


def attention_kernel(layer, *rest):
    small, rest = rest[:9], rest[9:]
    if layer:
        (k_raw, v_raw, wq, wk, wv, wo, k_first, v_first, x_out, u_out, gate_out, ko_hbm, vo_hbm, kbuf, vbuf, q_rows, k_t, v_t, o_rows, cos_t, sin_t, score, first_sem, cache_sem) = rest
    else:
        (kc_hbm, vc_hbm, wq_hbm, wk_hbm, wv_hbm, wo_hbm, x_out, u_out, gate_out, kbuf, vbuf, wq, wk, wv, wo, q_rows, k_t, v_t, o_rows, cos_t, sin_t, score, w_sem, cache_sem, *held, small_sem) = rest
        k_raw, v_raw = kbuf, vbuf
        small_copies = [pltpu.make_async_copy(src, dst, small_sem.at[i]) for i, (src, dst) in enumerate(zip(small, held))]
        small = held
        for copy in small_copies:
            copy.start()
    x_ref, again_ref, pos_ref, freq_ref, qgain_ref, kgain_ref, mgain_ref, ids_ref, wr_ref = small
    heads, slots, dim, rows = kbuf.shape
    half = dim // 2
    row = slice(layer, layer + 1)
    if layer:
        first_out = [pltpu.make_async_copy(src.at[n], dst.at[0, :, n], first_sem.at[i, n]) for n in range(heads) for i, (src, dst) in enumerate(((k_first, ko_hbm), (v_first, vo_hbm)))]
        for copy in first_out:
            copy.start()
    else:
        w_copies = [pltpu.make_async_copy(src.at[layer], dst, w_sem.at[i]) for i, (src, dst) in enumerate(((wq_hbm, wq), (wk_hbm, wk), (wv_hbm, wv), (wo_hbm, wo)))]
        for copy in w_copies[:3]:
            copy.start()

    def cache_copies(n):
        if layer:
            return (pltpu.make_async_copy(kbuf.at[n], ko_hbm.at[layer, :, n], cache_sem.at[0, n]), pltpu.make_async_copy(vbuf.at[n], vo_hbm.at[layer, :, n], cache_sem.at[1, n]))
        return (pltpu.make_async_copy(kc_hbm.at[layer, :, n], kbuf.at[n], cache_sem.at[0, n]), pltpu.make_async_copy(vc_hbm.at[layer, :, n], vbuf.at[n], cache_sem.at[1, n]))

    if not layer:
        for n in range(heads):
            for copy in cache_copies(n):
                copy.start()
        w_copies[3].start()

    if not layer:
        for copy in small_copies[:4]:
            copy.wait()
    pos = pos_ref[...]
    angles = pos.astype(F32) * freq_ref[...]
    cos_t[...] = jnp.cos(angles)
    sin_t[...] = jnp.sin(angles)
    normed = rms_scale(x_ref[...].astype(F32), again_ref[row]).astype(BF16)

    def rope(tensor):
        lo, hi = tensor[:half], tensor[half:]
        cos, sin = cos_t[...], sin_t[...]
        return jnp.concatenate([lo * cos - hi * sin, hi * cos + lo * sin], axis=0)

    if not layer:
        for copy in small_copies[4:]:
            copy.wait()
        w_copies[0].wait()
    q_rows[...] = rms_scale(jnp.dot(normed, wq[...], preferred_element_type=F32), qgain_ref[row])
    if not layer:
        w_copies[1].wait()
    key_new = rms_scale(jnp.dot(normed, wk[...], preferred_element_type=F32), kgain_ref[row])
    if not layer:
        w_copies[2].wait()
    value_new = jnp.dot(normed, wv[...], preferred_element_type=F32)
    pair = 2 * dim
    for c in range(heads // 2):
        chunk = key_new[:, c * pair:(c + 1) * pair].T
        for j in range(2):
            k_t[2 * c + j] = rope(chunk[j * dim:(j + 1) * dim]).astype(BF16)
        chunk = value_new[:, c * pair:(c + 1) * pair].T.astype(BF16)
        for j in range(2):
            v_t[2 * c + j] = chunk[j * dim:(j + 1) * dim]

    pos_b = jnp.broadcast_to(pos.astype(F32), (dim, rows)).astype(BF16)
    slot_ids = lax.broadcasted_iota(jnp.int32, (slots, rows), 0)

    def one_head(n, carry):
        cols = pl.ds(pl.multiple_of(n * pair, pair), pair)
        qt = q_rows[:, cols].T
        q0 = rope(qt[:dim]).astype(BF16).astype(F32) * dim ** -0.5
        q1 = rope(qt[dim:]).astype(BF16).astype(F32) * dim ** -0.5
        k_new, v_new = k_t[n], v_t[n]
        k_copy, v_copy = cache_copies(n)
        if not layer:
            k_copy.wait()
        for s in range(slots):
            key = jnp.where(pos_b == s, k_new, k_raw[n, s])
            kbuf[n, s] = key
            key = key.astype(F32)
            score[0, s:s + 1] = jnp.sum(key * q0, axis=0, keepdims=True)
            score[1, s:s + 1] = jnp.sum(key * q1, axis=0, keepdims=True)
        if layer:
            k_copy.start()
        for g in range(2):
            masked = jnp.where(slot_ids <= pos, score[g], -jnp.inf)
            weight = jnp.exp(masked - jnp.max(masked, axis=0, keepdims=True))
            score[g] = (weight / jnp.sum(weight, axis=0, keepdims=True)).astype(BF16).astype(F32)
        if not layer:
            v_copy.wait()
        acc0 = jnp.zeros((dim, rows), F32)
        acc1 = jnp.zeros((dim, rows), F32)
        for s in range(slots):
            value = jnp.where(pos_b == s, v_new, v_raw[n, s])
            vbuf[n, s] = value
            value = value.astype(F32)
            acc0 += value * score[0, s:s + 1]
            acc1 += value * score[1, s:s + 1]
        if layer:
            v_copy.start()
        o_rows[:, cols] = jnp.concatenate([acc0, acc1], axis=0).T.astype(BF16)
        return carry

    lax.fori_loop(0, heads, one_head, 0)
    if not layer:
        w_copies[3].wait()
    x_new = (x_ref[...].astype(F32) + jnp.dot(o_rows[...], wo[...], preferred_element_type=F32)).astype(BF16)
    x_out[...] = x_new
    u = rms_scale(x_new.astype(F32), mgain_ref[row]).astype(BF16)
    u_out[...] = u
    logits = lax.dot_general(wr_ref[layer], u, (((1,), (1,)), ((), ())), preferred_element_type=F32)
    weight = jnp.exp(logits - jnp.max(logits, axis=0, keepdims=True))
    probs = weight / jnp.sum(weight, axis=0, keepdims=True)
    expert_ids = lax.broadcasted_iota(jnp.int32, probs.shape, 0)
    member = expert_ids == ids_ref[layer, 0:1]
    for j in range(1, ids_ref.shape[1]):
        member = member | (expert_ids == ids_ref[layer, j:j + 1])
    gate_out[...] = jnp.where(member, probs, 0.0)
    if layer:
        for copy in first_out:
            copy.wait()
        for n in range(heads):
            for copy in cache_copies(n):
                copy.wait()


def attention_call(layer, x, pos, freq, ids, again, qgain, kgain, mgain, wr, kc, vc, wq, wk, wv, wo, ready):
    layers, slots, heads, dim, rows = kc.shape
    hidden = x.shape[1]
    experts = wr.shape[1]
    q_width, kv_width = wq.shape[2], wk.shape[2]
    vmem, hbm = pl.BlockSpec(memory_space=pltpu.VMEM), pl.BlockSpec(memory_space=pltpu.HBM)
    small = (x, again, pos, freq, qgain, kgain, mgain, ids, wr)
    out_shape = [
        jax.ShapeDtypeStruct((rows, hidden), BF16),
        jax.ShapeDtypeStruct((rows, hidden), BF16),
        jax.ShapeDtypeStruct((experts, rows), F32),
    ]
    cache = pltpu.VMEM((heads, slots, dim, rows), BF16)
    dma = pltpu.SemaphoreType.DMA
    scratch = [
        pltpu.VMEM((rows, q_width), F32),
        pltpu.VMEM((heads, dim, rows), BF16),
        pltpu.VMEM((heads, dim, rows), BF16),
        pltpu.VMEM((rows, q_width), BF16),
        pltpu.VMEM((dim // 2, rows), F32),
        pltpu.VMEM((dim // 2, rows), F32),
        pltpu.VMEM((2, slots, rows), F32),
    ]
    if layer:
        args = small + tuple(pltpu.with_memory_space_constraint(a, pltpu.VMEM) for a in ready)
        in_specs = [vmem] * len(args)
        out_shape += [jax.ShapeDtypeStruct(kc.shape, kc.dtype), jax.ShapeDtypeStruct(vc.shape, vc.dtype)]
        out_specs = [vmem] * 3 + [hbm] * 2
        scratch = [cache, cache] + scratch + [dma((2, heads)), dma((2, heads))]
    else:
        args = tuple(pltpu.with_memory_space_constraint(a, pltpu.HBM) for a in small) + (kc, vc, wq, wk, wv, wo)
        in_specs = [hbm] * len(args)
        out_shape += [cache, cache]
        out_specs = [vmem] * 5
        scratch = [pltpu.VMEM(w.shape[1:], BF16) for w in (wq, wk, wv, wo)] + scratch + [dma((4,)), dma((2, heads))] + [pltpu.VMEM(a.shape, a.dtype) for a in small] + [dma((len(small),))]
    return pl.pallas_call(
        functools.partial(attention_kernel, layer),
        name=f"attention_{layer}",
        out_shape=out_shape,
        in_specs=in_specs,
        out_specs=out_specs,
        scratch_shapes=scratch,
        compiler_params=pltpu.CompilerParams(vmem_limit_bytes=ATTENTION_VMEM),
    )(*args)


def moe_kernel(layer, n_ahead, u_ref, gate_ref, x_ref, wg_hbm, wu_hbm, wd_hbm, *rest):
    ahead_hbm, out_ref, ahead, rest = rest[:n_ahead], rest[n_ahead], rest[n_ahead + 1:2 * n_ahead + 1], rest[2 * n_ahead + 1:]
    (wg, wu, wd, ag_u, ag_g, part, psib, rs_in, w_sem, agu_send, agu_recv, sbu_send, sbu_recv, agg_send, agg_recv, sbg_send, sbg_recv, ps_send, ps_recv, rs_send, rs_recv, ahead_sem) = rest
    steps, _, rows, hidden = part.shape
    me = lax.axis_index("ep")
    core, chip = me % 2, me // 2
    chip_z, chip_y = chip // 2, chip % 2
    place = chip_y * (steps - 1 - chip_z) + (1 - chip_y) * chip_z

    def device_at(p, c):
        far = p // (steps // 2)
        z = (1 - far) * p + far * (steps - 1 - p)
        return (z * 2 + far) * 2 + c

    nxt = device_at((place + 1 - 2 * core + steps) % steps, core)
    prv = device_at((place - 1 + 2 * core + steps) % steps, core)
    sib = chip * 2 + (1 - core)

    w_copies = [pltpu.make_async_copy(src.at[layer], dst, w_sem.at[i]) for i, (src, dst) in enumerate(((wg_hbm, wg), (wu_hbm, wu), (wd_hbm, wd)))]
    for copy in w_copies:
        copy.start()
    barrier = pltpu.get_barrier_semaphore()
    for peer in (prv, sib):
        pl.semaphore_signal(barrier, inc=1, device_id={"ep": peer}, device_id_type=MESH)

    def remote(src, dst, send, recv, peer):
        return pltpu.make_async_remote_copy(src_ref=src, dst_ref=dst, send_sem=send, recv_sem=recv, device_id={"ep": peer}, device_id_type=MESH)

    ag_rows = rows // AG_SUBS
    rs_rows = rows // RS_SUBS

    def ring_u(k, s, src=None):
        span = pl.ds(s * ag_rows, ag_rows)
        src = ag_u.at[k, 0, span] if src is None else src.at[span]
        return remote(src, ag_u.at[k + 1, 0, span], agu_send.at[k, s], agu_recv.at[k + 1, s], nxt)

    def sib_u(k, s, src=None):
        span = pl.ds(s * ag_rows, ag_rows)
        src = ag_u.at[k, 0, span] if src is None else src.at[span]
        return remote(src, ag_u.at[k, 1, span], sbu_send.at[k, s], sbu_recv.at[k, s], sib)

    def ring_g(k, src=None):
        return remote(ag_g.at[k, 0] if src is None else src, ag_g.at[k + 1, 0], agg_send.at[k], agg_recv.at[k + 1], nxt)

    def sib_g(k, src=None):
        return remote(ag_g.at[k, 0] if src is None else src, ag_g.at[k, 1], sbg_send.at[k], sbg_recv.at[k], sib)

    def sib_part(k, s):
        span = pl.ds(s * rs_rows, rs_rows)
        return remote(part.at[k, 1, span], psib.at[k, span], ps_send.at[k, s], ps_recv.at[k, s], sib)

    def ring_part(k, s):
        span = pl.ds(s * rs_rows, rs_rows)
        return remote(part.at[k, 0, span], rs_in.at[k, span], rs_send.at[k, s], rs_recv.at[k, s], nxt)

    pl.semaphore_wait(barrier, 2)
    ring_g(0, gate_ref).start()
    for s in range(AG_SUBS):
        ring_u(0, s, u_ref).start()
    sib_g(0, gate_ref).start()
    for s in range(AG_SUBS):
        sib_u(0, s, u_ref).start()
    ag_u[0, 0] = u_ref[...]
    ag_g[0, 0] = gate_ref[...]

    def take_sub(k, s):
        if s == 0:
            ring_g(k - 1).wait_recv()

            @pl.when(k < steps - 1)
            def _():
                ring_g(k).start()

            sib_g(k).start()
        ring_u(k - 1, s).wait_recv()

        @pl.when(k < steps - 1)
        def _():
            ring_u(k, s).start()

        sib_u(k, s).start()

    def add_sub(k, s, first):
        span = pl.ds(s * rs_rows, rs_rows)
        sib_part(k, s).wait_recv()
        total = part[k, 0, span] + psib[k, span]
        if not first:
            ring_part(k - 1, s).wait_recv()
            total += rs_in[k - 1, span]
        part[k, 0, span] = total
        ring_part(k, s).start()

    lane = lax.broadcasted_iota(jnp.int32, (rows, gate_ref.shape[0]), 1)
    for copy in w_copies:
        copy.wait()
    ahead_copies = []
    for i, (src, dst) in enumerate(zip(ahead_hbm, ahead)):
        if len(src.shape) == 3:
            ahead_copies.append(pltpu.make_async_copy(src.at[layer + 1], dst, ahead_sem.at[i, 0]))
        else:
            ahead_copies += [pltpu.make_async_copy(src.at[layer + 1, :, n], dst.at[n], ahead_sem.at[i, n]) for n in range(dst.shape[0])]
    for copy in ahead_copies:
        copy.start()

    def one_step(k, carry):
        def forward(s):
            @pl.when(k < steps - 1)
            def _():
                take_sub(k + 1, s)

        def reduce(s):
            @pl.when(k == 2)
            def _():
                add_sub(k - 1, s, True)

            @pl.when(k > 2)
            def _():
                add_sub(k - 1, s, False)

        forward(0)
        sib_g(k).wait_recv()
        for s in range(AG_SUBS):
            sib_u(k, s).wait_recv()
        block = ag_u[k].reshape(2 * rows, hidden)
        gates = [ag_g[k, j].T for j in range(2)]

        for e in range(2):
            gate_part = jnp.dot(block, wg[e], preferred_element_type=F32)
            up_part = jnp.dot(block, wu[e], preferred_element_type=F32)
            weight = jnp.concatenate([jnp.sum(jnp.where(lane == 2 * me + e, g, 0.0), axis=1, keepdims=True) for g in gates], axis=0)
            activated = jnp.where(weight != 0.0, jax.nn.silu(gate_part) * up_part, 0.0).astype(BF16)
            forward(2 * e + 1)
            reduce(2 * e)
            expert_out = jnp.dot(activated, wd[e], preferred_element_type=F32).astype(BF16).astype(F32) * weight
            expert_out = expert_out.reshape(2, rows, hidden)
            if e == 0:
                part[k] = expert_out
            else:
                part[k] += expert_out
            if e == 0:
                forward(2)
            reduce(2 * e + 1)
        for s in range(RS_SUBS):
            sib_part(k, s).start()
        return carry

    lax.fori_loop(0, steps, one_step, 0)
    for s in range(RS_SUBS):
        add_sub(steps - 1, s, False)
    for s in range(RS_SUBS):
        span = pl.ds(s * rs_rows, rs_rows)
        sib_part(0, s).wait_recv()
        own = part[0, 0, span] + psib[0, span]
        ring_part(steps - 1, s).wait_recv()
        out_ref[span] = (x_ref[span].astype(F32) + (own + rs_in[steps - 1, span])).astype(BF16)

    def drain(k, carry):
        sib_g(k).wait_send()
        for s in range(AG_SUBS):
            sib_u(k, s).wait_send()
        for s in range(RS_SUBS):
            sib_part(k, s).wait_send()

        @pl.when(k < steps - 1)
        def _():
            ring_g(k).wait_send()
            for s in range(AG_SUBS):
                ring_u(k, s).wait_send()
            for s in range(RS_SUBS):
                ring_part(k + 1, s).wait_send()

        return carry

    lax.fori_loop(0, steps, drain, 0)
    for copy in ahead_copies:
        copy.wait()


def moe_call(layer, u, gate, x, wg, wu, wd, steps, ahead):
    rows, hidden = u.shape
    experts = gate.shape[0]
    width = wg.shape[3]
    vmem, hbm = pl.BlockSpec(memory_space=pltpu.VMEM), pl.BlockSpec(memory_space=pltpu.HBM)
    dma = pltpu.SemaphoreType.DMA
    kept = [a.shape[1:] if a.ndim == 3 else (a.shape[2], a.shape[1]) + a.shape[3:] for a in ahead]
    return pl.pallas_call(
        functools.partial(moe_kernel, layer, len(ahead)),
        name=f"moe_{layer}",
        out_shape=[jax.ShapeDtypeStruct((rows, hidden), BF16)] + [pltpu.VMEM(shape, BF16) for shape in kept],
        in_specs=[vmem] * 3 + [hbm] * (3 + len(ahead)),
        out_specs=[vmem] * (1 + len(ahead)),
        scratch_shapes=[
            pltpu.VMEM((2, hidden, width), BF16),
            pltpu.VMEM((2, hidden, width), BF16),
            pltpu.VMEM((2, width, hidden), BF16),
            pltpu.VMEM((steps, 2, rows, hidden), BF16),
            pltpu.VMEM((steps, 2, experts, rows), F32),
            pltpu.VMEM((steps, 2, rows, hidden), F32),
            pltpu.VMEM((steps, rows, hidden), F32),
            pltpu.VMEM((steps, rows, hidden), F32),
            dma((3,)),
            dma((steps, AG_SUBS)), dma((steps, AG_SUBS)), dma((steps, AG_SUBS)), dma((steps, AG_SUBS)),
            dma((steps,)), dma((steps,)), dma((steps,)), dma((steps,)),
            dma((steps, RS_SUBS)), dma((steps, RS_SUBS)), dma((steps, RS_SUBS)), dma((steps, RS_SUBS)),
            dma((6, 8)),
        ],
        compiler_params=pltpu.CompilerParams(vmem_limit_bytes=MOE_VMEM, collective_id=layer, has_side_effects=True),
    )(u, gate, x, wg, wu, wd, *ahead)


def solution(mesh):
    group_size = mesh.shape['ep']
    seq_axes = ('dp', 'ep')

    def device_step(hidden_state, key_cache, value_cache, positions, expert_ids, attn_gain, w_query, w_key, w_value, q_gain, k_gain, w_out, moe_gain, w_router, w_gate, w_up, w_down):
        dim = key_cache.shape[-1]
        rows = hidden_state.shape[0]
        freq = np.float32(ROPE_THETA) ** (-np.arange(0, dim, 2, dtype=np.float32) / np.float32(dim))
        freq = np.ascontiguousarray(np.broadcast_to(freq.astype(np.float32)[:, None], (dim // 2, rows)))
        keys = jnp.transpose(key_cache, (0, 2, 3, 4, 1))
        values = jnp.transpose(value_cache, (0, 2, 3, 4, 1))
        ids = jnp.transpose(expert_ids, (0, 2, 1))
        router = jnp.transpose(w_router, (0, 2, 1))
        pos = positions[None, :]
        small = (pos, freq, ids, attn_gain, q_gain, k_gain, moe_gain, router)
        big = tuple(pltpu.with_memory_space_constraint(a, pltpu.HBM) for a in (keys, values, w_query, w_key, w_value, w_out))
        experts = tuple(pltpu.with_memory_space_constraint(a, pltpu.HBM) for a in (w_gate, w_up, w_down)) + (group_size // 2,)
        hidden_x, u, gate, *first = attention_call(0, hidden_state, *small, *big, ())
        hidden_x, *ready = moe_call(0, u, gate, hidden_x, *experts, big)
        hidden_x, u, gate, *prev = attention_call(1, hidden_x, *small, *big, (*ready, *first))
        hidden_x, = moe_call(1, u, gate, hidden_x, *experts, ())
        return hidden_x, jnp.transpose(prev[0], (0, 4, 1, 2, 3)), jnp.transpose(prev[1], (0, 4, 1, 2, 3))

    cache_spec = P(None, seq_axes, None, None, None)
    expert_spec = P(None, 'ep', None, None)
    in_specs = (P(seq_axes, None), cache_spec, cache_spec, P(seq_axes), P(None, seq_axes, None)) + (P(),) * 9 + (expert_spec,) * 3
    out_specs = (P(seq_axes, None), cache_spec, cache_spec)
    return jax.shard_map(device_step, mesh=mesh, in_specs=in_specs, out_specs=out_specs, check_vma=False)
```

```python
import functools

import jax
import jax.numpy as jnp
from jax import lax
from jax.experimental import pallas as pl
from jax.experimental.pallas import tpu as pltpu
from jax.sharding import PartitionSpec as P
import numpy as np

NORM_EPS = 1e-5
ROPE_THETA = 10000.0
F32 = jnp.float32
BF16 = jnp.bfloat16
MESH = pl.DeviceIdType.MESH
RS_SUBS = 4
AG_SUBS = 4
ATTENTION_VMEM = 16 * 1024 * 1024
MOE_VMEM = 32 * 1024 * 1024
FIRST_VMEM = 31 * 1024 * 1024


def turns(subs, part):
    return range(part * subs // 4, (part + 1) * subs // 4)


def rms_scale(tensor, gain):
    mean_sq = jnp.mean(tensor * tensor, axis=-1, keepdims=True)
    return tensor * lax.rsqrt(mean_sq + NORM_EPS) * gain


def attention_kernel(layer, *rest, loading=None):
    small, rest = rest[:9], rest[9:]
    if layer:
        (k_raw, v_raw, wq, wk, wv, wo, k_first, v_first, x_out, u_out, gate_out, ko_hbm, vo_hbm, kbuf, vbuf, q_rows, k_t, v_t, o_rows, cos_t, sin_t, score, first_sem, cache_sem) = rest
    else:
        (kc_hbm, vc_hbm, wq_hbm, wk_hbm, wv_hbm, wo_hbm, x_out, u_out, gate_out, kbuf, vbuf, wq, wk, wv, wo, q_rows, k_t, v_t, o_rows, cos_t, sin_t, score, w_sem, cache_sem, *held, small_sem) = rest
        k_raw, v_raw = kbuf, vbuf
        small_copies = [pltpu.make_async_copy(src, dst, small_sem.at[i]) for i, (src, dst) in enumerate(zip(small, held))]
        small = held
        for copy in small_copies:
            copy.start()
    x_ref, again_ref, pos_ref, freq_ref, qgain_ref, kgain_ref, mgain_ref, ids_ref, wr_ref = small
    heads, slots, dim, rows = kbuf.shape
    half = dim // 2
    row = slice(layer, layer + 1)
    if layer:
        first_out = [pltpu.make_async_copy(src.at[n], dst.at[0, :, n], first_sem.at[i, n]) for n in range(heads) for i, (src, dst) in enumerate(((k_first, ko_hbm), (v_first, vo_hbm)))]
        for copy in first_out:
            copy.start()
    else:
        w_copies = [pltpu.make_async_copy(src.at[layer], dst, w_sem.at[i]) for i, (src, dst) in enumerate(((wq_hbm, wq), (wk_hbm, wk), (wv_hbm, wv), (wo_hbm, wo)))]
        for copy in w_copies[:3]:
            copy.start()

    def cache_copies(n):
        if layer:
            return (pltpu.make_async_copy(kbuf.at[n], ko_hbm.at[layer, :, n], cache_sem.at[0, n]), pltpu.make_async_copy(vbuf.at[n], vo_hbm.at[layer, :, n], cache_sem.at[1, n]))
        return (pltpu.make_async_copy(kc_hbm.at[layer, :, n], kbuf.at[n], cache_sem.at[0, n]), pltpu.make_async_copy(vc_hbm.at[layer, :, n], vbuf.at[n], cache_sem.at[1, n]))

    if not layer:
        for copy in small_copies[:4]:
            copy.wait()
    pos = pos_ref[...]
    angles = pos.astype(F32) * freq_ref[...]
    cos_t[...] = jnp.cos(angles)
    sin_t[...] = jnp.sin(angles)
    normed = rms_scale(x_ref[...].astype(F32), again_ref[row]).astype(BF16)

    def rope(tensor):
        lo, hi = tensor[:half], tensor[half:]
        cos, sin = cos_t[...], sin_t[...]
        return jnp.concatenate([lo * cos - hi * sin, hi * cos + lo * sin], axis=0)

    if not layer:
        for copy in small_copies[4:]:
            copy.wait()
        w_copies[0].wait()
        w_copies[1].wait()
        w_copies[2].wait()
        for n in range(heads):
            for copy in cache_copies(n):
                copy.start()
        w_copies[3].start()
        loading()
    q_rows[...] = rms_scale(jnp.dot(normed, wq[...], preferred_element_type=F32), qgain_ref[row])
    key_new = rms_scale(jnp.dot(normed, wk[...], preferred_element_type=F32), kgain_ref[row])
    value_new = jnp.dot(normed, wv[...], preferred_element_type=F32)
    pair = 2 * dim
    for c in range(heads // 2):
        chunk = key_new[:, c * pair:(c + 1) * pair].T
        for j in range(2):
            k_t[2 * c + j] = rope(chunk[j * dim:(j + 1) * dim]).astype(BF16)
        chunk = value_new[:, c * pair:(c + 1) * pair].T.astype(BF16)
        for j in range(2):
            v_t[2 * c + j] = chunk[j * dim:(j + 1) * dim]

    pos_b = jnp.broadcast_to(pos.astype(F32), (dim, rows)).astype(BF16)
    slot_ids = lax.broadcasted_iota(jnp.int32, (slots, rows), 0)

    def one_head(n, carry):
        cols = pl.ds(pl.multiple_of(n * pair, pair), pair)
        qt = q_rows[:, cols].T
        q0 = rope(qt[:dim]).astype(BF16).astype(F32) * dim ** -0.5
        q1 = rope(qt[dim:]).astype(BF16).astype(F32) * dim ** -0.5
        k_new, v_new = k_t[n], v_t[n]
        k_copy, v_copy = cache_copies(n)
        if not layer:
            k_copy.wait()
        for s in range(slots):
            key = jnp.where(pos_b == s, k_new, k_raw[n, s])
            kbuf[n, s] = key
            key = key.astype(F32)
            score[0, s:s + 1] = jnp.sum(key * q0, axis=0, keepdims=True)
            score[1, s:s + 1] = jnp.sum(key * q1, axis=0, keepdims=True)
        if layer:
            k_copy.start()
        for g in range(2):
            masked = jnp.where(slot_ids <= pos, score[g], -jnp.inf)
            weight = jnp.exp(masked - jnp.max(masked, axis=0, keepdims=True))
            score[g] = (weight / jnp.sum(weight, axis=0, keepdims=True)).astype(BF16).astype(F32)
        if not layer:
            v_copy.wait()
        acc0 = jnp.zeros((dim, rows), F32)
        acc1 = jnp.zeros((dim, rows), F32)
        for s in range(slots):
            value = jnp.where(pos_b == s, v_new, v_raw[n, s])
            vbuf[n, s] = value
            value = value.astype(F32)
            acc0 += value * score[0, s:s + 1]
            acc1 += value * score[1, s:s + 1]
        if layer:
            v_copy.start()
        o_rows[:, cols] = jnp.concatenate([acc0, acc1], axis=0).T.astype(BF16)
        return carry

    lax.fori_loop(0, heads, one_head, 0)
    if not layer:
        w_copies[3].wait()
    x_new = (x_ref[...].astype(F32) + jnp.dot(o_rows[...], wo[...], preferred_element_type=F32)).astype(BF16)
    x_out[...] = x_new
    u = rms_scale(x_new.astype(F32), mgain_ref[row]).astype(BF16)
    u_out[...] = u
    logits = lax.dot_general(wr_ref[layer], u, (((1,), (1,)), ((), ())), preferred_element_type=F32)
    weight = jnp.exp(logits - jnp.max(logits, axis=0, keepdims=True))
    probs = weight / jnp.sum(weight, axis=0, keepdims=True)
    expert_ids = lax.broadcasted_iota(jnp.int32, probs.shape, 0)
    ids = ids_ref[layer]
    picked = jnp.concatenate([jnp.sum(jnp.where(expert_ids == ids[j:j + 1], probs, 0.0), axis=0, keepdims=True) for j in range(ids.shape[0])], axis=0)
    ids = ids.astype(F32)
    low = lax.broadcasted_iota(jnp.int32, ids.shape, 1) < rows // 2
    gate_out[0] = jnp.where(low, picked, pltpu.roll(ids, rows // 2, 1))
    gate_out[1] = jnp.where(low, pltpu.roll(picked, rows // 2, 1), ids)
    if layer:
        for copy in first_out:
            copy.wait()
        for n in range(heads):
            for copy in cache_copies(n):
                copy.wait()


def attention_call(small, keys, values, ready):
    rows, hidden = small[0].shape
    _, slots, heads, dim, _ = keys.shape
    gate_shape = (2, small[7].shape[1], rows)
    vmem, hbm = pl.BlockSpec(memory_space=pltpu.VMEM), pl.BlockSpec(memory_space=pltpu.HBM)
    dma = pltpu.SemaphoreType.DMA
    args = tuple(pltpu.with_memory_space_constraint(a, pltpu.VMEM) for a in small[:1]) + small[1:] + tuple(pltpu.with_memory_space_constraint(a, pltpu.VMEM) for a in ready)
    cache = pltpu.VMEM((heads, slots, dim, rows), BF16)
    return pl.pallas_call(
        functools.partial(attention_kernel, 1),
        name="attention_1",
        out_shape=[
            jax.ShapeDtypeStruct((rows, hidden), BF16),
            jax.ShapeDtypeStruct((rows, hidden), BF16),
            jax.ShapeDtypeStruct(gate_shape, F32),
            jax.ShapeDtypeStruct(keys.shape, keys.dtype),
            jax.ShapeDtypeStruct(values.shape, values.dtype),
        ],
        in_specs=[vmem] * len(args),
        out_specs=[vmem] * 3 + [hbm] * 2,
        scratch_shapes=[cache, cache] + attention_scratch(rows, ready[2].shape[1], heads, dim, slots) + [dma((2, heads)), dma((2, heads))],
        compiler_params=pltpu.CompilerParams(vmem_limit_bytes=ATTENTION_VMEM),
    )(*args)


def moe_kernel(layer, n_ahead, u_ref, gate_ref, x_ref, wg_hbm, wu_hbm, wd_hbm, *rest, first=None):
    ahead_hbm, out_ref, ahead, rest = rest[:n_ahead], rest[n_ahead], rest[n_ahead + 1:2 * n_ahead + 1], rest[2 * n_ahead + 1:]
    (wg, wu, wd, ag_u, ag_g, part, psib, rs_in, w_sem, agu_send, agu_recv, sbu_send, sbu_recv, agg_send, agg_recv, sbg_send, sbg_recv, ps_send, ps_recv, rs_send, rs_recv, ahead_sem) = rest
    steps, _, rows, hidden = part.shape
    me = lax.axis_index("ep")
    core, chip = me % 2, me // 2
    chip_z, chip_y = chip // 2, chip % 2
    place = chip_y * (steps - 1 - chip_z) + (1 - chip_y) * chip_z

    def device_at(p, c):
        far = p // (steps // 2)
        z = (1 - far) * p + far * (steps - 1 - p)
        return (z * 2 + far) * 2 + c

    nxt = device_at((place + 1 - 2 * core + steps) % steps, core)
    prv = device_at((place - 1 + 2 * core + steps) % steps, core)
    sib = chip * 2 + (1 - core)

    w_copies = [pltpu.make_async_copy(src.at[layer], dst, w_sem.at[i]) for i, (src, dst) in enumerate(((wg_hbm, wg), (wu_hbm, wu), (wd_hbm, wd)))]

    def load_experts():
        for copy in w_copies:
            copy.start()

    barrier = pltpu.get_barrier_semaphore()
    for peer in (prv, sib):
        pl.semaphore_signal(barrier, inc=1, device_id={"ep": peer}, device_id_type=MESH)

    def remote(src, dst, send, recv, peer):
        return pltpu.make_async_remote_copy(src_ref=src, dst_ref=dst, send_sem=send, recv_sem=recv, device_id={"ep": peer}, device_id_type=MESH)

    ag_rows = rows // AG_SUBS
    rs_rows = rows // RS_SUBS

    def ring_u(k, s, src=None):
        span = pl.ds(s * ag_rows, ag_rows)
        src = ag_u.at[k, 0, span] if src is None else src.at[span]
        return remote(src, ag_u.at[k + 1, 0, span], agu_send.at[k, s], agu_recv.at[k + 1, s], nxt)

    def sib_u(k, s, src=None):
        span = pl.ds(s * ag_rows, ag_rows)
        src = ag_u.at[k, 0, span] if src is None else src.at[span]
        return remote(src, ag_u.at[k, 1, span], sbu_send.at[k, s], sbu_recv.at[k, s], sib)

    def ring_g(k, src=None):
        return remote(ag_g.at[k, 0] if src is None else src, ag_g.at[k + 1, 0], agg_send.at[k], agg_recv.at[k + 1], nxt)

    def sib_g(k, src=None):
        return remote(ag_g.at[k, 0] if src is None else src, ag_g.at[k, 1], sbg_send.at[k], sbg_recv.at[k], sib)

    def sib_part(k, s):
        span = pl.ds(s * rs_rows, rs_rows)
        return remote(part.at[k, 1, span], psib.at[k, span], ps_send.at[k, s], ps_recv.at[k, s], sib)

    def ring_part(k, s):
        span = pl.ds(s * rs_rows, rs_rows)
        return remote(part.at[k, 0, span], rs_in.at[k, span], rs_send.at[k, s], rs_recv.at[k, s], nxt)

    if first is None:
        load_experts()
    else:
        first(load_experts)
    pl.semaphore_wait(barrier, 2)
    ring_g(0, gate_ref).start()
    for turn in range(4):
        for s in turns(AG_SUBS, turn):
            ring_u(0, s, u_ref).start()
    sib_g(0, gate_ref).start()
    for s in range(AG_SUBS):
        sib_u(0, s, u_ref).start()
    ag_u[0, 0] = u_ref[...]
    ag_g[0, 0] = gate_ref[...]

    def take_sub(k, s):
        if s == 0:
            ring_g(k - 1).wait_recv()

            @pl.when(k < steps - 1)
            def _():
                ring_g(k).start()

            sib_g(k).start()
        ring_u(k - 1, s).wait_recv()

        @pl.when(k < steps - 1)
        def _():
            ring_u(k, s).start()

        sib_u(k, s).start()

    def add_sub(k, s, first):
        span = pl.ds(s * rs_rows, rs_rows)
        sib_part(k, s).wait_recv()
        total = part[k, 0, span] + psib[k, span]
        if not first:
            ring_part(k - 1, s).wait_recv()
            total += rs_in[k - 1, span]
        part[k, 0, span] = total
        ring_part(k, s).start()

    low = lax.broadcasted_iota(jnp.int32, (1, rows), 1) < rows // 2
    for copy in w_copies:
        copy.wait()
    ahead_copies = []
    for i, (src, dst) in enumerate(zip(ahead_hbm, ahead)):
        if len(src.shape) == 3:
            ahead_copies.append(pltpu.make_async_copy(src.at[layer + 1], dst, ahead_sem.at[i, 0]))
        else:
            ahead_copies += [pltpu.make_async_copy(src.at[layer + 1, :, n], dst.at[n], ahead_sem.at[i, n]) for n in range(dst.shape[0])]
    for copy in ahead_copies:
        copy.start()

    def one_step(k, carry):
        def forward(turn):
            @pl.when(k < steps - 1)
            def _():
                for s in turns(AG_SUBS, turn):
                    take_sub(k + 1, s)

        def reduce(turn):
            @pl.when(k == 2)
            def _():
                for s in turns(RS_SUBS, turn):
                    add_sub(k - 1, s, True)

            @pl.when(k > 2)
            def _():
                for s in turns(RS_SUBS, turn):
                    add_sub(k - 1, s, False)

        forward(0)
        sib_g(k).wait_recv()
        for s in range(AG_SUBS):
            sib_u(k, s).wait_recv()
        block = ag_u[k].reshape(2 * rows, hidden)
        weights = []
        for e in range(2):
            for j in range(2):
                halves = []
                for h in range(2):
                    table = ag_g[k, j, h]
                    wanted = pltpu.roll(table, rows // 2, 1) == (2 * me + e).astype(F32)
                    halves.append(jnp.sum(jnp.where(wanted, table, 0.0), axis=0, keepdims=True))
                weights.append(jnp.where(low, halves[0], pltpu.roll(halves[1], rows // 2, 1)))
        columns = jnp.concatenate(weights + weights, axis=0).T

        for e in range(2):
            gate_part = jnp.dot(block, wg[e], preferred_element_type=F32)
            up_part = jnp.dot(block, wu[e], preferred_element_type=F32)
            weight = jnp.concatenate([columns[:, 2 * e + j:2 * e + j + 1] for j in range(2)], axis=0)
            activated = jnp.where(weight != 0.0, jax.nn.silu(gate_part) * up_part, 0.0).astype(BF16)
            forward(2 * e + 1)
            reduce(2 * e)
            expert_out = jnp.dot(activated, wd[e], preferred_element_type=F32).astype(BF16).astype(F32) * weight
            expert_out = expert_out.reshape(2, rows, hidden)
            if e == 0:
                part[k] = expert_out
            else:
                part[k] += expert_out
            if e == 0:
                forward(2)
            reduce(2 * e + 1)
        for s in range(RS_SUBS):
            sib_part(k, s).start()
        return carry

    lax.fori_loop(0, steps, one_step, 0)
    for turn in range(4):
        for s in turns(RS_SUBS, turn):
            add_sub(steps - 1, s, False)
    for s in [s for turn in range(4) for s in turns(RS_SUBS, turn)]:
        span = pl.ds(s * rs_rows, rs_rows)
        sib_part(0, s).wait_recv()
        own = part[0, 0, span] + psib[0, span]
        ring_part(steps - 1, s).wait_recv()
        out_ref[span] = (x_ref[span].astype(F32) + (own + rs_in[steps - 1, span])).astype(BF16)

    def drain(k, carry):
        sib_g(k).wait_send()
        for s in range(AG_SUBS):
            sib_u(k, s).wait_send()
        for s in range(RS_SUBS):
            sib_part(k, s).wait_send()

        @pl.when(k < steps - 1)
        def _():
            ring_g(k).wait_send()
            for s in range(AG_SUBS):
                ring_u(k, s).wait_send()
            for s in range(RS_SUBS):
                ring_part(k + 1, s).wait_send()

        return carry

    lax.fori_loop(0, steps, drain, 0)
    for copy in ahead_copies:
        copy.wait()


def first_kernel(n_small, n_big, n_experts, n_out, n_attention, *refs):
    it = iter(refs)
    small, big, experts, outs, scratch, state = ([next(it) for _ in range(n)] for n in (n_small, n_big, n_experts, n_out, n_attention, 3))
    out_ref, kbuf, vbuf, *ahead = outs
    x_ref, u_ref, gate_ref = state

    def first(loading):
        attention_kernel(0, *small, *big, x_ref, u_ref, gate_ref, kbuf, vbuf, *ahead[2:], *scratch, loading=loading)

    moe_kernel(0, n_big, u_ref, gate_ref, x_ref, *experts, *big, out_ref, *ahead, *it, first=first)


def attention_scratch(rows, q_width, heads, dim, slots):
    return [
        pltpu.VMEM((rows, q_width), F32),
        pltpu.VMEM((heads, dim, rows), BF16),
        pltpu.VMEM((heads, dim, rows), BF16),
        pltpu.VMEM((rows, q_width), BF16),
        pltpu.VMEM((dim // 2, rows), F32),
        pltpu.VMEM((dim // 2, rows), F32),
        pltpu.VMEM((2, slots, rows), F32),
    ]


def moe_scratch(rows, hidden, width, gate_shape, steps, n_heads):
    dma = pltpu.SemaphoreType.DMA
    return [
        pltpu.VMEM((2, hidden, width), BF16),
        pltpu.VMEM((2, hidden, width), BF16),
        pltpu.VMEM((2, width, hidden), BF16),
        pltpu.VMEM((steps, 2, rows, hidden), BF16),
        pltpu.VMEM((steps, 2) + gate_shape, F32),
        pltpu.VMEM((steps, 2, rows, hidden), F32),
        pltpu.VMEM((steps, rows, hidden), F32),
        pltpu.VMEM((steps, rows, hidden), F32),
        dma((3,)),
        dma((steps, AG_SUBS)), dma((steps, AG_SUBS)), dma((steps, AG_SUBS)), dma((steps, AG_SUBS)),
        dma((steps,)), dma((steps,)), dma((steps,)), dma((steps,)),
        dma((steps, RS_SUBS)), dma((steps, RS_SUBS)), dma((steps, RS_SUBS)), dma((steps, RS_SUBS)),
        dma((6, n_heads)),
    ]


def first_call(small, big, experts, steps):
    rows, hidden = small[0].shape
    keys, w_query = big[0], big[2]
    _, slots, heads, dim, _ = keys.shape
    gate_shape = (2, small[7].shape[1], rows)
    hbm, vmem = pl.BlockSpec(memory_space=pltpu.HBM), pl.BlockSpec(memory_space=pltpu.VMEM)
    dma = pltpu.SemaphoreType.DMA
    cache = pltpu.VMEM((heads, slots, dim, rows), BF16)
    out_shape = [pltpu.VMEM((rows, hidden), BF16)] + [cache] * 4 + [pltpu.VMEM(w.shape[1:], BF16) for w in big[2:]]
    scratch = attention_scratch(rows, w_query.shape[2], heads, dim, slots) + [dma((4,)), dma((2, heads))] + [pltpu.VMEM(a.shape, a.dtype) for a in small] + [dma((len(small),))]
    state = [pltpu.VMEM((rows, hidden), BF16), pltpu.VMEM((rows, hidden), BF16), pltpu.VMEM(gate_shape, F32)]
    args = tuple(pltpu.with_memory_space_constraint(a, pltpu.HBM) for a in small) + big + experts
    return pl.pallas_call(
        functools.partial(first_kernel, len(small), len(big), len(experts), len(out_shape), len(scratch)),
        name="attention_moe_0",
        out_shape=out_shape,
        in_specs=[hbm] * len(args),
        out_specs=[vmem] * len(out_shape),
        scratch_shapes=scratch + state + moe_scratch(rows, hidden, experts[0].shape[3], gate_shape, steps, heads),
        compiler_params=pltpu.CompilerParams(vmem_limit_bytes=FIRST_VMEM, collective_id=0, has_side_effects=True),
    )(*args)


def moe_call(u, gate, x, wg, wu, wd, steps, heads):
    rows, hidden = u.shape
    vmem, hbm = pl.BlockSpec(memory_space=pltpu.VMEM), pl.BlockSpec(memory_space=pltpu.HBM)
    return pl.pallas_call(
        functools.partial(moe_kernel, 1, 0),
        name="moe_1",
        out_shape=jax.ShapeDtypeStruct((rows, hidden), BF16),
        in_specs=[vmem] * 3 + [hbm] * 3,
        out_specs=vmem,
        scratch_shapes=moe_scratch(rows, hidden, wg.shape[3], gate.shape, steps, heads),
        compiler_params=pltpu.CompilerParams(vmem_limit_bytes=MOE_VMEM, collective_id=1, has_side_effects=True),
    )(u, gate, x, wg, wu, wd)


def solution(mesh):
    group_size = mesh.shape['ep']
    seq_axes = ('dp', 'ep')

    def device_step(hidden_state, key_cache, value_cache, positions, expert_ids, attn_gain, w_query, w_key, w_value, q_gain, k_gain, w_out, moe_gain, w_router, w_gate, w_up, w_down):
        dim = key_cache.shape[-1]
        rows = hidden_state.shape[0]
        freq = np.float32(ROPE_THETA) ** (-np.arange(0, dim, 2, dtype=np.float32) / np.float32(dim))
        freq = np.ascontiguousarray(np.broadcast_to(freq.astype(np.float32)[:, None], (dim // 2, rows)))
        keys = jnp.transpose(key_cache, (0, 2, 3, 4, 1))
        values = jnp.transpose(value_cache, (0, 2, 3, 4, 1))
        ids = jnp.transpose(expert_ids, (0, 2, 1))
        router = jnp.transpose(w_router, (0, 2, 1))
        pos = positions[None, :]
        small = (attn_gain, pos, freq, q_gain, k_gain, moe_gain, ids, router)
        big = tuple(pltpu.with_memory_space_constraint(a, pltpu.HBM) for a in (keys, values, w_query, w_key, w_value, w_out))
        experts = tuple(pltpu.with_memory_space_constraint(a, pltpu.HBM) for a in (w_gate, w_up, w_down))
        hidden_x, k_first, v_first, *ready = first_call((hidden_state,) + small, big, experts, group_size // 2)
        hidden_x, u, gate, *prev = attention_call((hidden_x,) + small, keys, values, (*ready, k_first, v_first))
        hidden_x = moe_call(u, gate, hidden_x, *experts, group_size // 2, key_cache.shape[3])
        return hidden_x, jnp.transpose(prev[0], (0, 4, 1, 2, 3)), jnp.transpose(prev[1], (0, 4, 1, 2, 3))

    cache_spec = P(None, seq_axes, None, None, None)
    expert_spec = P(None, 'ep', None, None)
    in_specs = (P(seq_axes, None), cache_spec, cache_spec, P(seq_axes), P(None, seq_axes, None)) + (P(),) * 9 + (expert_spec,) * 3
    out_specs = (P(seq_axes, None), cache_spec, cache_spec)
    return jax.shard_map(device_step, mesh=mesh, in_specs=in_specs, out_specs=out_specs, check_vma=False)
```

```python
import functools

import jax
import jax.numpy as jnp
from jax import lax
from jax.experimental import pallas as pl
from jax.experimental.pallas import tpu as pltpu
from jax.sharding import PartitionSpec as P
import numpy as np

NORM_EPS = 1e-5
ROPE_THETA = 10000.0
F32 = jnp.float32
BF16 = jnp.bfloat16
MESH = pl.DeviceIdType.MESH
RS_SUBS = 4
AG_SUBS = 4
ATTENTION_VMEM = 16 * 1024 * 1024
MOE_VMEM = 32 * 1024 * 1024
FIRST_VMEM = 31 * 1024 * 1024


def turns(subs, part):
    return range(part * subs // 4, (part + 1) * subs // 4)


def rms_scale(tensor, gain):
    mean_sq = jnp.mean(tensor * tensor, axis=-1, keepdims=True)
    return tensor * lax.rsqrt(mean_sq + NORM_EPS) * gain


def spread_positions(pos, dim):
    return jnp.broadcast_to(pos.astype(F32), (dim, pos.shape[1])).astype(BF16)


def attention_kernel(layer, *rest, loading=None):
    small, rest = rest[:9], rest[9:]
    if layer:
        (k_raw, v_raw, wq, wk, wv, wo, k_first, v_first, x_out, u_out, gate_out, ko_hbm, vo_hbm, kbuf, vbuf, q_rows, k_t, v_t, o_rows, cos_t, sin_t, score, first_sem, cache_sem) = rest
    else:
        (kc_hbm, vc_hbm, wq_hbm, wk_hbm, wv_hbm, wo_hbm, x_out, u_out, gate_out, kbuf, vbuf, wq, wk, wv, wo, q_rows, k_t, v_t, o_rows, cos_t, sin_t, score, w_sem, cache_sem, *held, small_sem) = rest
        k_raw, v_raw = kbuf, vbuf
        small_copies = [pltpu.make_async_copy(src, dst, small_sem.at[i]) for i, (src, dst) in enumerate(zip(small, held))]
        small = held
        for copy in small_copies:
            copy.start()
    x_ref, again_ref, pos_ref, freq_ref, qgain_ref, kgain_ref, mgain_ref, ids_ref, wr_ref = small
    heads, slots, dim, rows = kbuf.shape
    half = dim // 2
    row = slice(layer, layer + 1)
    if layer:
        first_out = [pltpu.make_async_copy(src.at[n], dst.at[0, :, n], first_sem.at[i, n]) for n in range(heads) for i, (src, dst) in enumerate(((k_first, ko_hbm), (v_first, vo_hbm)))]
        for copy in first_out:
            copy.start()
    else:
        w_copies = [pltpu.make_async_copy(src.at[layer], dst, w_sem.at[i]) for i, (src, dst) in enumerate(((wq_hbm, wq), (wk_hbm, wk), (wv_hbm, wv), (wo_hbm, wo)))]
        for copy in w_copies[:3]:
            copy.start()

    def cache_copies(n):
        if layer:
            return (pltpu.make_async_copy(kbuf.at[n], ko_hbm.at[layer, :, n], cache_sem.at[0, n]), pltpu.make_async_copy(vbuf.at[n], vo_hbm.at[layer, :, n], cache_sem.at[1, n]))
        return (pltpu.make_async_copy(kc_hbm.at[layer, :, n], kbuf.at[n], cache_sem.at[0, n]), pltpu.make_async_copy(vc_hbm.at[layer, :, n], vbuf.at[n], cache_sem.at[1, n]))

    if not layer:
        for copy in small_copies[:4]:
            copy.wait()
    pos = pos_ref[...]
    angles = pos.astype(F32) * freq_ref[...]
    cos_t[...] = jnp.cos(angles)
    sin_t[...] = jnp.sin(angles)
    normed = rms_scale(x_ref[...].astype(F32), again_ref[row]).astype(BF16)

    def rope(tensor):
        lo, hi = tensor[:half], tensor[half:]
        cos, sin = cos_t[...], sin_t[...]
        return jnp.concatenate([lo * cos - hi * sin, hi * cos + lo * sin], axis=0)

    if not layer:
        for copy in small_copies[4:]:
            copy.wait()
        w_copies[0].wait()
        w_copies[1].wait()
        w_copies[2].wait()
        for n in range(heads):
            for copy in cache_copies(n):
                copy.start()
        w_copies[3].start()
        loading()
    q_rows[...] = rms_scale(jnp.dot(normed, wq[...], preferred_element_type=F32), qgain_ref[row])
    key_new = rms_scale(jnp.dot(normed, wk[...], preferred_element_type=F32), kgain_ref[row])
    value_new = jnp.dot(normed, wv[...], preferred_element_type=F32)
    pair = 2 * dim
    for c in range(heads // 2):
        chunk = key_new[:, c * pair:(c + 1) * pair].T
        for j in range(2):
            k_t[2 * c + j] = rope(chunk[j * dim:(j + 1) * dim]).astype(BF16)
        chunk = value_new[:, c * pair:(c + 1) * pair].T.astype(BF16)
        for j in range(2):
            v_t[2 * c + j] = chunk[j * dim:(j + 1) * dim]

    pos_b = spread_positions(pos, dim)
    slot_ids = lax.broadcasted_iota(jnp.int32, score.shape[1:], 0)
    visible = slot_ids <= pos if layer else (slot_ids < pos) | (slot_ids == slots)

    def one_head(n, carry):
        cols = pl.ds(pl.multiple_of(n * pair, pair), pair)
        qt = q_rows[:, cols].T
        q0 = rope(qt[:dim]).astype(BF16).astype(F32) * dim ** -0.5
        q1 = rope(qt[dim:]).astype(BF16).astype(F32) * dim ** -0.5
        k_new, v_new = k_t[n], v_t[n]
        k_copy, v_copy = cache_copies(n)
        if not layer:
            k_copy.wait()
        for s in range(slots):
            key = k_raw[n, s]
            if layer:
                key = jnp.where(pos_b == s, k_new, key)
                kbuf[n, s] = key
            key = key.astype(F32)
            score[0, s:s + 1] = jnp.sum(key * q0, axis=0, keepdims=True)
            score[1, s:s + 1] = jnp.sum(key * q1, axis=0, keepdims=True)
        if layer:
            k_copy.start()
        else:
            key = k_new.astype(F32)
            score[0, slots:slots + 1] = jnp.sum(key * q0, axis=0, keepdims=True)
            score[1, slots:slots + 1] = jnp.sum(key * q1, axis=0, keepdims=True)
        for g in range(2):
            masked = jnp.where(visible, score[g], -jnp.inf)
            weight = jnp.exp(masked - jnp.max(masked, axis=0, keepdims=True))
            score[g] = (weight / jnp.sum(weight, axis=0, keepdims=True)).astype(BF16).astype(F32)
        if not layer:
            v_copy.wait()
        acc0 = jnp.zeros((dim, rows), F32)
        acc1 = jnp.zeros((dim, rows), F32)
        for s in range(slots):
            value = v_raw[n, s]
            if layer:
                value = jnp.where(pos_b == s, v_new, value)
                vbuf[n, s] = value
            value = value.astype(F32)
            acc0 += value * score[0, s:s + 1]
            acc1 += value * score[1, s:s + 1]
        if not layer:
            value = v_new.astype(F32)
            acc0 += value * score[0, slots:slots + 1]
            acc1 += value * score[1, slots:slots + 1]
        if layer:
            v_copy.start()
        o_rows[:, cols] = jnp.concatenate([acc0, acc1], axis=0).T.astype(BF16)
        return carry

    lax.fori_loop(0, heads, one_head, 0)
    if not layer:
        w_copies[3].wait()
    x_new = (x_ref[...].astype(F32) + jnp.dot(o_rows[...], wo[...], preferred_element_type=F32)).astype(BF16)
    x_out[...] = x_new
    u = rms_scale(x_new.astype(F32), mgain_ref[row]).astype(BF16)
    u_out[...] = u
    logits = lax.dot_general(wr_ref[layer], u, (((1,), (1,)), ((), ())), preferred_element_type=F32)
    weight = jnp.exp(logits - jnp.max(logits, axis=0, keepdims=True))
    probs = weight / jnp.sum(weight, axis=0, keepdims=True)
    expert_ids = lax.broadcasted_iota(jnp.int32, probs.shape, 0)
    ids = ids_ref[layer]
    picked = jnp.concatenate([jnp.sum(jnp.where(expert_ids == ids[j:j + 1], probs, 0.0), axis=0, keepdims=True) for j in range(ids.shape[0])], axis=0)
    ids = ids.astype(F32)
    low = lax.broadcasted_iota(jnp.int32, ids.shape, 1) < rows // 2
    gate_out[0] = jnp.where(low, picked, pltpu.roll(ids, rows // 2, 1))
    gate_out[1] = jnp.where(low, pltpu.roll(picked, rows // 2, 1), ids)
    if layer:
        for copy in first_out:
            copy.wait()
        for n in range(heads):
            for copy in cache_copies(n):
                copy.wait()


def attention_call(small, keys, values, ready):
    rows, hidden = small[0].shape
    _, slots, heads, dim, _ = keys.shape
    gate_shape = (2, small[7].shape[1], rows)
    vmem, hbm = pl.BlockSpec(memory_space=pltpu.VMEM), pl.BlockSpec(memory_space=pltpu.HBM)
    dma = pltpu.SemaphoreType.DMA
    args = tuple(pltpu.with_memory_space_constraint(a, pltpu.VMEM) for a in small[:1]) + small[1:] + tuple(pltpu.with_memory_space_constraint(a, pltpu.VMEM) for a in ready)
    cache = pltpu.VMEM((heads, slots, dim, rows), BF16)
    return pl.pallas_call(
        functools.partial(attention_kernel, 1),
        name="attention_1",
        out_shape=[
            jax.ShapeDtypeStruct((rows, hidden), BF16),
            jax.ShapeDtypeStruct((rows, hidden), BF16),
            jax.ShapeDtypeStruct(gate_shape, F32),
            jax.ShapeDtypeStruct(keys.shape, keys.dtype),
            jax.ShapeDtypeStruct(values.shape, values.dtype),
        ],
        in_specs=[vmem] * len(args),
        out_specs=[vmem] * 3 + [hbm] * 2,
        scratch_shapes=[cache, cache] + attention_scratch(rows, ready[2].shape[1], heads, dim, slots) + [dma((2, heads)), dma((2, heads))],
        compiler_params=pltpu.CompilerParams(vmem_limit_bytes=ATTENTION_VMEM),
    )(*args)


def moe_kernel(layer, n_ahead, u_ref, gate_ref, x_ref, wg_hbm, wu_hbm, wd_hbm, *rest, first=None, idle=None):
    ahead_hbm, out_ref, ahead, rest = rest[:n_ahead], rest[n_ahead], rest[n_ahead + 1:2 * n_ahead + 1], rest[2 * n_ahead + 1:]
    (wg, wu, wd, ag_u, ag_g, part, psib, rs_in, w_sem, agu_send, agu_recv, sbu_send, sbu_recv, agg_send, agg_recv, sbg_send, sbg_recv, ps_send, ps_recv, rs_send, rs_recv, ahead_sem) = rest
    steps, _, rows, hidden = part.shape
    me = lax.axis_index("ep")
    core, chip = me % 2, me // 2
    chip_z, chip_y = chip // 2, chip % 2
    place = chip_y * (steps - 1 - chip_z) + (1 - chip_y) * chip_z

    def device_at(p, c):
        far = p // (steps // 2)
        z = (1 - far) * p + far * (steps - 1 - p)
        return (z * 2 + far) * 2 + c

    nxt = device_at((place + 1 - 2 * core + steps) % steps, core)
    prv = device_at((place - 1 + 2 * core + steps) % steps, core)
    sib = chip * 2 + (1 - core)

    w_copies = [pltpu.make_async_copy(src.at[layer], dst, w_sem.at[i]) for i, (src, dst) in enumerate(((wg_hbm, wg), (wu_hbm, wu), (wd_hbm, wd)))]

    def load_experts():
        for copy in w_copies:
            copy.start()

    barrier = pltpu.get_barrier_semaphore()
    for peer in (prv, sib):
        pl.semaphore_signal(barrier, inc=1, device_id={"ep": peer}, device_id_type=MESH)

    def remote(src, dst, send, recv, peer):
        return pltpu.make_async_remote_copy(src_ref=src, dst_ref=dst, send_sem=send, recv_sem=recv, device_id={"ep": peer}, device_id_type=MESH)

    ag_rows = rows // AG_SUBS
    rs_rows = rows // RS_SUBS

    def ring_u(k, s, src=None):
        span = pl.ds(s * ag_rows, ag_rows)
        src = ag_u.at[k, 0, span] if src is None else src.at[span]
        return remote(src, ag_u.at[k + 1, 0, span], agu_send.at[k, s], agu_recv.at[k + 1, s], nxt)

    def sib_u(k, s, src=None):
        span = pl.ds(s * ag_rows, ag_rows)
        src = ag_u.at[k, 0, span] if src is None else src.at[span]
        return remote(src, ag_u.at[k, 1, span], sbu_send.at[k, s], sbu_recv.at[k, s], sib)

    def ring_g(k, src=None):
        return remote(ag_g.at[k, 0] if src is None else src, ag_g.at[k + 1, 0], agg_send.at[k], agg_recv.at[k + 1], nxt)

    def sib_g(k, src=None):
        return remote(ag_g.at[k, 0] if src is None else src, ag_g.at[k, 1], sbg_send.at[k], sbg_recv.at[k], sib)

    def sib_part(k, s):
        span = pl.ds(s * rs_rows, rs_rows)
        return remote(part.at[k, 1, span], psib.at[k, span], ps_send.at[k, s], ps_recv.at[k, s], sib)

    def ring_part(k, s):
        span = pl.ds(s * rs_rows, rs_rows)
        return remote(part.at[k, 0, span], rs_in.at[k, span], rs_send.at[k, s], rs_recv.at[k, s], nxt)

    if first is None:
        load_experts()
    else:
        first(load_experts)
    pl.semaphore_wait(barrier, 2)
    ring_g(0, gate_ref).start()
    for turn in range(4):
        for s in turns(AG_SUBS, turn):
            ring_u(0, s, u_ref).start()
    sib_g(0, gate_ref).start()
    for s in range(AG_SUBS):
        sib_u(0, s, u_ref).start()
    ag_u[0, 0] = u_ref[...]
    ag_g[0, 0] = gate_ref[...]

    def take_sub(k, s):
        if s == 0:
            ring_g(k - 1).wait_recv()

            @pl.when(k < steps - 1)
            def _():
                ring_g(k).start()

            sib_g(k).start()
        ring_u(k - 1, s).wait_recv()

        @pl.when(k < steps - 1)
        def _():
            ring_u(k, s).start()

        sib_u(k, s).start()

    def add_sub(k, s, first):
        span = pl.ds(s * rs_rows, rs_rows)
        sib_part(k, s).wait_recv()
        total = part[k, 0, span] + psib[k, span]
        if not first:
            ring_part(k - 1, s).wait_recv()
            total += rs_in[k - 1, span]
        part[k, 0, span] = total
        ring_part(k, s).start()

    low = lax.broadcasted_iota(jnp.int32, (1, rows), 1) < rows // 2
    for copy in w_copies:
        copy.wait()
    ahead_copies = []
    for i, (src, dst) in enumerate(zip(ahead_hbm, ahead)):
        if len(src.shape) == 3:
            ahead_copies.append(pltpu.make_async_copy(src.at[layer + 1], dst, ahead_sem.at[i, 0]))
        else:
            ahead_copies += [pltpu.make_async_copy(src.at[layer + 1, :, n], dst.at[n], ahead_sem.at[i, n]) for n in range(dst.shape[0])]
    for copy in ahead_copies:
        copy.start()

    def one_step(k, carry):
        def forward(turn):
            @pl.when(k < steps - 1)
            def _():
                for s in turns(AG_SUBS, turn):
                    take_sub(k + 1, s)

        def reduce(turn):
            @pl.when(k == 2)
            def _():
                for s in turns(RS_SUBS, turn):
                    add_sub(k - 1, s, True)

            @pl.when(k > 2)
            def _():
                for s in turns(RS_SUBS, turn):
                    add_sub(k - 1, s, False)

        forward(0)
        sib_g(k).wait_recv()
        for s in range(AG_SUBS):
            sib_u(k, s).wait_recv()
        block = ag_u[k].reshape(2 * rows, hidden)
        weights = []
        for e in range(2):
            for j in range(2):
                halves = []
                for h in range(2):
                    table = ag_g[k, j, h]
                    wanted = pltpu.roll(table, rows // 2, 1) == (2 * me + e).astype(F32)
                    halves.append(jnp.sum(jnp.where(wanted, table, 0.0), axis=0, keepdims=True))
                weights.append(jnp.where(low, halves[0], pltpu.roll(halves[1], rows // 2, 1)))
        columns = jnp.concatenate(weights + weights, axis=0).T

        for e in range(2):
            gate_part = jnp.dot(block, wg[e], preferred_element_type=F32)
            up_part = jnp.dot(block, wu[e], preferred_element_type=F32)
            weight = jnp.concatenate([columns[:, 2 * e + j:2 * e + j + 1] for j in range(2)], axis=0)
            activated = jnp.where(weight != 0.0, jax.nn.silu(gate_part) * up_part, 0.0).astype(BF16)
            forward(2 * e + 1)
            reduce(2 * e)
            expert_out = jnp.dot(activated, wd[e], preferred_element_type=F32).astype(BF16).astype(F32) * weight
            expert_out = expert_out.reshape(2, rows, hidden)
            if e == 0:
                part[k] = expert_out
            else:
                part[k] += expert_out
            if e == 0:
                forward(2)
            reduce(2 * e + 1)
            if e == 0 and idle is not None:
                idle(k, 0)
        for s in range(RS_SUBS):
            sib_part(k, s).start()
        if idle is not None:
            idle(k, 1)
        return carry

    lax.fori_loop(0, steps, one_step, 0)
    for turn in range(4):
        for s in turns(RS_SUBS, turn):
            add_sub(steps - 1, s, False)
    for s in [s for turn in range(4) for s in turns(RS_SUBS, turn)]:
        span = pl.ds(s * rs_rows, rs_rows)
        sib_part(0, s).wait_recv()
        own = part[0, 0, span] + psib[0, span]
        ring_part(steps - 1, s).wait_recv()
        out_ref[span] = (x_ref[span].astype(F32) + (own + rs_in[steps - 1, span])).astype(BF16)

    def drain(k, carry):
        sib_g(k).wait_send()
        for s in range(AG_SUBS):
            sib_u(k, s).wait_send()
        for s in range(RS_SUBS):
            sib_part(k, s).wait_send()

        @pl.when(k < steps - 1)
        def _():
            ring_g(k).wait_send()
            for s in range(AG_SUBS):
                ring_u(k, s).wait_send()
            for s in range(RS_SUBS):
                ring_part(k + 1, s).wait_send()

        return carry

    lax.fori_loop(0, steps, drain, 0)
    for copy in ahead_copies:
        copy.wait()


def first_kernel(n_small, n_big, n_experts, n_out, n_attention, *refs):
    it = iter(refs)
    small, big, experts, outs, scratch, state = ([next(it) for _ in range(n)] for n in (n_small, n_big, n_experts, n_out, n_attention, 3))
    out_ref, kbuf, vbuf, *ahead = outs
    x_ref, u_ref, gate_ref = state

    def first(loading):
        attention_kernel(0, *small, *big, x_ref, u_ref, gate_ref, kbuf, vbuf, *ahead[2:], *scratch, loading=loading)

    heads, slots, dim, _ = kbuf.shape
    k_t, v_t, pos_ref = scratch[1], scratch[2], scratch[11]

    def idle(k, turn):
        @pl.when((k >= 3) & (k < 3 + heads // 2))
        def _():
            n = 2 * (k - 3) + turn
            pos_b = spread_positions(pos_ref[...], dim)
            for s in range(slots):
                for buf, new in ((kbuf, k_t), (vbuf, v_t)):
                    buf[n, s] = jnp.where(pos_b == s, new[n], buf[n, s])

    moe_kernel(0, n_big, u_ref, gate_ref, x_ref, *experts, *big, out_ref, *ahead, *it, first=first, idle=idle)


def attention_scratch(rows, q_width, heads, dim, score_rows):
    return [
        pltpu.VMEM((rows, q_width), F32),
        pltpu.VMEM((heads, dim, rows), BF16),
        pltpu.VMEM((heads, dim, rows), BF16),
        pltpu.VMEM((rows, q_width), BF16),
        pltpu.VMEM((dim // 2, rows), F32),
        pltpu.VMEM((dim // 2, rows), F32),
        pltpu.VMEM((2, score_rows, rows), F32),
    ]


def moe_scratch(rows, hidden, width, gate_shape, steps, n_heads):
    dma = pltpu.SemaphoreType.DMA
    return [
        pltpu.VMEM((2, hidden, width), BF16),
        pltpu.VMEM((2, hidden, width), BF16),
        pltpu.VMEM((2, width, hidden), BF16),
        pltpu.VMEM((steps, 2, rows, hidden), BF16),
        pltpu.VMEM((steps, 2) + gate_shape, F32),
        pltpu.VMEM((steps, 2, rows, hidden), F32),
        pltpu.VMEM((steps, rows, hidden), F32),
        pltpu.VMEM((steps, rows, hidden), F32),
        dma((3,)),
        dma((steps, AG_SUBS)), dma((steps, AG_SUBS)), dma((steps, AG_SUBS)), dma((steps, AG_SUBS)),
        dma((steps,)), dma((steps,)), dma((steps,)), dma((steps,)),
        dma((steps, RS_SUBS)), dma((steps, RS_SUBS)), dma((steps, RS_SUBS)), dma((steps, RS_SUBS)),
        dma((6, n_heads)),
    ]


def first_call(small, big, experts, steps):
    rows, hidden = small[0].shape
    keys, w_query = big[0], big[2]
    _, slots, heads, dim, _ = keys.shape
    gate_shape = (2, small[7].shape[1], rows)
    hbm, vmem = pl.BlockSpec(memory_space=pltpu.HBM), pl.BlockSpec(memory_space=pltpu.VMEM)
    dma = pltpu.SemaphoreType.DMA
    cache = pltpu.VMEM((heads, slots, dim, rows), BF16)
    out_shape = [pltpu.VMEM((rows, hidden), BF16)] + [cache] * 4 + [pltpu.VMEM(w.shape[1:], BF16) for w in big[2:]]
    scratch = attention_scratch(rows, w_query.shape[2], heads, dim, slots + 8) + [dma((4,)), dma((2, heads))] + [pltpu.VMEM(a.shape, a.dtype) for a in small] + [dma((len(small),))]
    state = [pltpu.VMEM((rows, hidden), BF16), pltpu.VMEM((rows, hidden), BF16), pltpu.VMEM(gate_shape, F32)]
    args = tuple(pltpu.with_memory_space_constraint(a, pltpu.HBM) for a in small) + big + experts
    return pl.pallas_call(
        functools.partial(first_kernel, len(small), len(big), len(experts), len(out_shape), len(scratch)),
        name="attention_moe_0",
        out_shape=out_shape,
        in_specs=[hbm] * len(args),
        out_specs=[vmem] * len(out_shape),
        scratch_shapes=scratch + state + moe_scratch(rows, hidden, experts[0].shape[3], gate_shape, steps, heads),
        compiler_params=pltpu.CompilerParams(vmem_limit_bytes=FIRST_VMEM, collective_id=0, has_side_effects=True),
    )(*args)


def moe_call(u, gate, x, wg, wu, wd, steps, heads):
    rows, hidden = u.shape
    vmem, hbm = pl.BlockSpec(memory_space=pltpu.VMEM), pl.BlockSpec(memory_space=pltpu.HBM)
    return pl.pallas_call(
        functools.partial(moe_kernel, 1, 0),
        name="moe_1",
        out_shape=jax.ShapeDtypeStruct((rows, hidden), BF16),
        in_specs=[vmem] * 3 + [hbm] * 3,
        out_specs=vmem,
        scratch_shapes=moe_scratch(rows, hidden, wg.shape[3], gate.shape, steps, heads),
        compiler_params=pltpu.CompilerParams(vmem_limit_bytes=MOE_VMEM, collective_id=1, has_side_effects=True),
    )(u, gate, x, wg, wu, wd)


def solution(mesh):
    group_size = mesh.shape['ep']
    seq_axes = ('dp', 'ep')

    def device_step(hidden_state, key_cache, value_cache, positions, expert_ids, attn_gain, w_query, w_key, w_value, q_gain, k_gain, w_out, moe_gain, w_router, w_gate, w_up, w_down):
        dim = key_cache.shape[-1]
        rows = hidden_state.shape[0]
        freq = np.float32(ROPE_THETA) ** (-np.arange(0, dim, 2, dtype=np.float32) / np.float32(dim))
        freq = np.ascontiguousarray(np.broadcast_to(freq.astype(np.float32)[:, None], (dim // 2, rows)))
        keys = jnp.transpose(key_cache, (0, 2, 3, 4, 1))
        values = jnp.transpose(value_cache, (0, 2, 3, 4, 1))
        ids = jnp.transpose(expert_ids, (0, 2, 1))
        router = jnp.transpose(w_router, (0, 2, 1))
        pos = positions[None, :]
        small = (attn_gain, pos, freq, q_gain, k_gain, moe_gain, ids, router)
        big = tuple(pltpu.with_memory_space_constraint(a, pltpu.HBM) for a in (keys, values, w_query, w_key, w_value, w_out))
        experts = tuple(pltpu.with_memory_space_constraint(a, pltpu.HBM) for a in (w_gate, w_up, w_down))
        hidden_x, k_first, v_first, *ready = first_call((hidden_state,) + small, big, experts, group_size // 2)
        hidden_x, u, gate, *prev = attention_call((hidden_x,) + small, keys, values, (*ready, k_first, v_first))
        hidden_x = moe_call(u, gate, hidden_x, *experts, group_size // 2, key_cache.shape[3])
        return hidden_x, jnp.transpose(prev[0], (0, 4, 1, 2, 3)), jnp.transpose(prev[1], (0, 4, 1, 2, 3))

    cache_spec = P(None, seq_axes, None, None, None)
    expert_spec = P(None, 'ep', None, None)
    in_specs = (P(seq_axes, None), cache_spec, cache_spec, P(seq_axes), P(None, seq_axes, None)) + (P(),) * 9 + (expert_spec,) * 3
    out_specs = (P(seq_axes, None), cache_spec, cache_spec)
    return jax.shard_map(device_step, mesh=mesh, in_specs=in_specs, out_specs=out_specs, check_vma=False)
```
